256 devices in a mesh: dom: 256 (over y, x, z, core).
Axes of the slice: x: 4, y: 4, z: 8, core: 2. Of those that a mesh axis runs over, the one named last changes fastest.
Arguments:
- currents: float32 [16, 524288], P(None, 'dom'), may hold values from -36 to 36
- conductance: float32 [524288], P('dom'), may hold values from 0.25 to 4
- ground: float32 [524288], P('dom'), may hold values from 0.1 to 1
- ell_cols: int32 [9, 524288], P(None, 'dom'), may hold values from -1 to 2815, as said below
- send_rows: int32 [1536, 128], P('dom'), may hold values from -1 to 2047, as said below
Outputs:
- voltages: float32 [16, 524288], P(None, 'dom')
- residual: float32 [16, 524288], P(None, 'dom')
The draws below stay inside these ranges and needn't reach their ends.
Inputs may be any that keep to these rules, and one draw needn't show every extreme that they name: `ell_cols`: column n belongs to the partition of node n. Entry -1 is an empty slot; an entry below 2048 names a node of the same partition other than n; an entry c of 2048 or more names boundary slot c - 2048 as in the reference program, and only slots that the neighbouring partition lists (entries not -1 in its row of send_rows). The graph is symmetric: node a names node b in as many slots as b names a, and the two edges of a boundary slot pair the k-th live entries of the rows of partitions p and p + e. Each node has at most one edge to another partition. `send_rows`: row 2 * 3 * p + o lists, for the o-th offset e of -3, ..., -1, 1, ..., 3, the local node numbers of partition p whose values partition p + e reads; live entries come first and the rest are -1. The rows of p toward p + e and of p + e toward p have the same number of live entries, at most 128; in every draw some pair of rows is full. A node appears at most once among its partition's rows. Rows toward partitions outside 0 to 255 are all -1.
All inputs are finite; a program needn't handle non-finite values.
Results may differ from the reference program's by a relative error of at most 0.00011.
Values sent between devices are 32-bit elements; how exact they have to be, the bound alone decides.
A program may use at most 64 MiB of HBM per device.

```python
import math
import jax
import jax.numpy as jnp
from jax import lax

NODE_DEV = 2048
PAIRS = 16
SLOTS = 9
REACH = 3
ITERS = 3
BND = 128
PARTITIONS = 256
NODES = 524288
LINKS = 1536


def graph_tables(key):
    circle_count = (SLOTS - 1) // 2
    link_count = 2 * REACH
    counts = jax.random.randint(jax.random.fold_in(key, 11), (PARTITIONS, REACH), BND // 3, BND + 1)
    chosen = jax.random.randint(jax.random.fold_in(key, 12), (), 0, PARTITIONS - 1)
    counts = counts.at[chosen, 0].set(BND)
    part_ids = jnp.arange(PARTITIONS, dtype=jnp.int32)
    reaches = jnp.arange(1, REACH + 1, dtype=jnp.int32)
    counts = jnp.where(part_ids[:, None] + reaches[None, :] < PARTITIONS, counts, 0)

    def one_partition(part_index):
        part_key = jax.random.fold_in(key, part_index + 1000)
        ordering = jax.random.permutation(jax.random.fold_in(part_key, 0), NODE_DEV).astype(jnp.int32)
        position = jnp.zeros((NODE_DEV,), jnp.int32).at[ordering].set(jnp.arange(NODE_DEV, dtype=jnp.int32))
        source_part = part_index - reaches[::-1]
        lower_count = jnp.where(source_part >= 0, counts[jnp.clip(source_part, 0, PARTITIONS - 1), reaches[::-1] - 1], 0)
        live_count = jnp.concatenate([lower_count, counts[part_index]])
        slot_ids = jnp.arange(BND, dtype=jnp.int32)
        send_table = jnp.where(slot_ids[None, :] < live_count[:, None], ordering[:link_count * BND].reshape(link_count, BND), -1)
        block_index = jnp.clip(position // BND, 0, link_count - 1)
        cross_live = (position < link_count * BND) & (position % BND < live_count[block_index])
        columns = []
        for circle_number in range(circle_count):
            circle_key = jax.random.fold_in(part_key, circle_number + 1)
            circle_cycle = jax.random.permutation(circle_key, NODE_DEV).astype(jnp.int32)
            circle_place = jnp.zeros((NODE_DEV,), jnp.int32).at[circle_cycle].set(jnp.arange(NODE_DEV, dtype=jnp.int32))
            kept_edge = jax.random.randint(jax.random.fold_in(circle_key, 99), (NODE_DEV,), 0, 4) > 0
            earlier = (circle_place + NODE_DEV - 1) % NODE_DEV
            columns.append(jnp.where(kept_edge[circle_place], circle_cycle[(circle_place + 1) % NODE_DEV], -1))
            columns.append(jnp.where(kept_edge[earlier], circle_cycle[earlier], -1))
        columns.append(jnp.where(cross_live, NODE_DEV + position, -1))
        return (jnp.stack(columns), send_table)
    column_tables, send_tables = jax.vmap(one_partition)(part_ids)
    ell_table = jnp.transpose(column_tables, (1, 0, 2)).reshape(SLOTS, NODES)
    return (ell_table.astype(jnp.int32), send_tables.reshape(LINKS, BND).astype(jnp.int32))


def draw_ell_cols(key, part):
    return graph_tables(jax.random.fold_in(key, 7))[0]


def draw_send_rows(key, part):
    return graph_tables(jax.random.fold_in(key, 7))[1]


def draw_currents(key, part):
    node_part = (jnp.arange(NODES, dtype=jnp.int32) // NODE_DEV).astype(jnp.float32)
    part_scale = 1.0 + 2.0 * node_part / max(PARTITIONS - 1, 1)
    pair_scale = jnp.exp(jax.random.uniform(jax.random.fold_in(key, 1), (PAIRS, 1), minval=math.log(0.3), maxval=math.log(3.0)))
    base_draw = jnp.clip(jax.random.normal(jax.random.fold_in(key, 2), (PAIRS, NODES)), -4.0, 4.0)
    return (base_draw * part_scale[None, :] * pair_scale).astype(jnp.float32)


def block_levels(rng, extent, shards, low, high):
    loudness, own = 1.0, jax.random.fold_in(rng, 6)
    for dim, blocks in shards:
        heights = jnp.exp(jax.random.uniform(jax.random.fold_in(own, dim), (blocks,), jnp.float32, low / len(shards), high / len(shards)))
        loudness = loudness * jnp.repeat(heights, extent[dim] // blocks).reshape([-1 if axis == dim else 1 for axis in range(len(extent))])
    return loudness


def setup_inputs(seed: int = 0) -> dict:
    key_list = jax.random.split(jax.random.key(seed), 6)
    return {
        "currents": draw_currents(jax.random.fold_in(key_list[5], 71), 0),
        "conductance": jnp.clip(jnp.exp(math.log(4.0) - 2.7725887 * jax.random.uniform(key_list[1], (NODES,), jnp.float32) ** block_levels(key_list[1], (NODES,), ((0, 256),), -0.2, 0.2)), 0.25, 4.0),
        "ground": jnp.clip(jnp.exp(math.log(1.0) - 2.3025851 * jax.random.uniform(key_list[2], (NODES,), jnp.float32) ** block_levels(key_list[2], (NODES,), ((0, 256),), -0.2, 0.2)), 0.1, 1.0),
        "ell_cols": draw_ell_cols(jax.random.fold_in(key_list[5], 71), 0),
        "send_rows": draw_send_rows(jax.random.fold_in(key_list[5], 71), 0),
    }


def neighbour_table(ell_cols, send_rows):
    link_count = 2 * REACH
    offsets = jnp.array(list(range(-REACH, 0)) + list(range(1, REACH + 1)), dtype=jnp.int32)
    node_part = (jnp.arange(NODES, dtype=jnp.int32) // NODE_DEV).astype(jnp.int32)
    present = ell_cols >= 0
    local_edge = ell_cols < NODE_DEV
    region = jnp.clip(ell_cols - NODE_DEV, 0, link_count * BND - 1).astype(jnp.int32)
    block_index = region // BND
    within = region % BND
    source_part = jnp.clip(node_part[None, :] + offsets[block_index], 0, PARTITIONS - 1).astype(jnp.int32)
    list_row = source_part * link_count + (link_count - 1 - block_index)
    remote = send_rows[list_row, within]
    target = jnp.where(local_edge, node_part[None, :] * NODE_DEV + ell_cols, source_part * NODE_DEV + remote)
    return jnp.where(present, target, 0).astype(jnp.int32), present


def operate(field, degree, weight, target):
    def add_slot(slot_index, running):
        return running + weight[slot_index][None, :] * jnp.take(field, target[slot_index], axis=1)

    beside = lax.fori_loop(0, SLOTS, add_slot, jnp.zeros_like(field))
    return degree[None, :] * field - beside


def reference(currents, conductance, ground, ell_cols, send_rows):
    target, present = neighbour_table(ell_cols, send_rows)
    weight = jnp.where(present, 0.5 * (conductance[None, :] + conductance[target]), 0.0)
    degree = ground + jnp.sum(weight, axis=0)
    voltages = jnp.zeros_like(currents)
    residual = currents
    direction = currents
    norm_now = jnp.sum(residual * residual, axis=1)
    for iteration in range(ITERS):
        image = operate(direction, degree, weight, target)
        step_size = norm_now / jnp.sum(direction * image, axis=1)
        voltages = voltages + step_size[:, None] * direction
        residual = residual - step_size[:, None] * image
        norm_next = jnp.sum(residual * residual, axis=1)
        direction = residual + (norm_next / norm_now)[:, None] * direction
        norm_now = norm_next
    return voltages, residual
```

```python
import functools

import jax
import jax.numpy as jnp
from jax import lax
from jax.experimental import pallas as pl
from jax.experimental.pallas import tpu as pltpu
from jax.sharding import PartitionSpec as P

MESH = pl.DeviceIdType.MESH
F32, BF16, I16, I32 = jnp.float32, jnp.bfloat16, jnp.int16, jnp.int32
LANES = 128
WIDE = 256


def pieces(x):
    high = x.astype(BF16)
    rest = x - high.astype(F32)
    mid = rest.astype(BF16)
    low = (rest - mid.astype(F32)).astype(BF16)
    return [high, mid, low]


def joined(y, first, rows):
    return (y[first + 2 * rows : first + 3 * rows] + y[first + rows : first + 2 * rows]) + y[first : first + rows]


def tiles(width):
    return [slice(i, i + LANES) for i in range(0, width, LANES)]


def kernel(
    parts, group, cur, cond, gnd, ell, send, volt, resid,
    adj, sel, v1, v2, v3, y0, y1, y2, diag, lhs, blhs, slhs, wsend, u0, u1, u2, t0, t1, t2,
    out0, out1, out2, in0, in1, in2, red, ex_send, ex_recv, red_send, red_recv,
):
    pairs, nodes = cur.shape
    slots = ell.shape[0]
    links = send.shape[0]
    bound = links * LANES
    reach = links // 2
    offsets = list(range(-reach, 0)) + list(range(1, reach + 1))
    me = lax.axis_index("dom")
    others = parts // group
    mine, place = me // group, me % group

    neighbours = [lax.rem(me + e + parts, parts) for e in offsets]
    near = [mine * group + lax.rem(place + d, group) for d in range(1, group)]
    far = [lax.rem(mine + d, others) * group + place for d in range(1, others)]

    barrier = pltpu.get_barrier_semaphore()
    for peer in neighbours + near + far:
        pl.semaphore_signal(barrier, inc=1, device_id={"dom": peer}, device_id_type=MESH)

    ones = jnp.ones((16, LANES), BF16)
    none = jnp.zeros((16, LANES), BF16)
    row_ids = lax.broadcasted_iota(I32, (16, LANES), 0).astype(I16)

    def spread(row):
        return jnp.broadcast_to(row, (16, LANES)).astype(I16)

    for o in range(links):
        listed = spread(send[o : o + 1, :])

        def fill_sel(i, _, listed=listed, o=o):
            for q in range(16):
                at = pl.multiple_of(i * 256 + q * 16, 16)
                ids = row_ids + at.astype(I16)
                sel[pl.ds(at, 16), o * LANES : (o + 1) * LANES] = jnp.where(listed == ids, ones, none)
            return 0

        lax.fori_loop(0, nodes // 256, fill_sel, 0)

    def picked(y_parts, rows):
        for i, piece in enumerate(y_parts):
            slhs[i * rows : (i + 1) * rows, :] = piece

    slhs[...] = jnp.zeros_like(slhs)
    picked(pieces(cur[...]), pairs)
    for i, piece in enumerate(pieces(cond[...])):
        slhs[3 * pairs + i : 3 * pairs + i + 1, :] = piece
    for b in range(0, bound, WIDE):
        y = jnp.dot(slhs[...], sel[:, b : b + WIDE], preferred_element_type=F32)
        u0[:, b : b + WIDE] = joined(y, 0, pairs)
        c_part = joined(y, 3 * pairs, 1)
        wsend[:, b : b + WIDE] = jnp.broadcast_to(c_part, (8, WIDE))
    for o in range(links):
        s = slice(o * LANES, (o + 1) * LANES)
        out0[o, 0:pairs, :] = u0[:, s]
        out0[o, pairs : pairs + 8, :] = wsend[:, s]

    def exchange(step, out, into):
        copies = []
        for o in range(links):
            copies.append(
                pltpu.make_async_remote_copy(
                    src_ref=out.at[o],
                    dst_ref=into.at[links - 1 - o],
                    send_sem=ex_send.at[step, o],
                    recv_sem=ex_recv.at[step, links - 1 - o],
                    device_id={"dom": neighbours[o]},
                    device_id_type=MESH,
                )
            )
        return copies

    def start(copies):
        for copy in copies:
            copy.start()

    def arrive(copies):
        for copy in copies:
            copy.wait_recv()

    pl.semaphore_wait(barrier, len(neighbours) + len(near) + len(far))
    ex0 = exchange(0, out0, in0)
    start(ex0)

    def build(t, _):
        off = pl.multiple_of(t * LANES, LANES)
        block = ell[:, pl.ds(off, LANES)]
        cols = [spread(block[s : s + 1, :]) for s in range(slots)]
        counts = []
        for s in range(slots):
            total = none
            for other in range(slots):
                total = total + jnp.where(cols[s] == cols[other], ones, none)
            counts.append(total)

        def fill(i, _):
            for q in range(16):
                at = pl.multiple_of(i * 256 + q * 16, 16)
                ids = row_ids + at.astype(I16)
                acc = none
                for s in range(slots):
                    acc = jnp.where(cols[s] == ids, counts[s], acc)
                adj[pl.ds(at, 16), pl.ds(off, LANES)] = acc
            return 0

        lax.fori_loop(0, nodes // 256, fill, 0)

        remote = spread(jnp.max(block, axis=0, keepdims=True))

        def fill_remote(i, _):
            for q in range(16):
                at = pl.multiple_of(nodes + i * 256 + q * 16, 16)
                ids = row_ids + at.astype(I16)
                adj[pl.ds(at, 16), pl.ds(off, LANES)] = jnp.where(remote == ids, ones, none)
            return 0

        lax.fori_loop(0, bound // 256, fill_remote, 0)
        return 0

    lax.fori_loop(0, nodes // LANES, build, 0)

    def split_field(v):
        for i, piece in enumerate(pieces(v)):
            lhs[i * pairs : (i + 1) * pairs, :] = piece
        for i, piece in enumerate(pieces(v * cond[...])):
            lhs[(3 + i) * pairs : (4 + i) * pairs, :] = piece

    half = 0.5

    def local_operator(v, y, first):
        rows = 7 * pairs if first else 6 * pairs
        for b in range(0, nodes, WIDE):
            s = slice(b, b + WIDE)
            prod = jnp.dot(lhs[0:rows, :], adj[0:nodes, s], preferred_element_type=F32)
            c = cond[:, s]
            if first:
                extra = prod[6 * pairs :]
                around = joined(extra, 0, 1)
                diag[:, s] = gnd[:, s] + half * (c * extra[3:4] + around)
            y[:, s] = diag[:, s] * v[:, s] - half * (c * joined(prod, 0, pairs) + joined(prod, 3 * pairs, pairs))

    def pick_listed(y, start_with):
        picked(pieces(y[...]), pairs)
        got = []
        for b in range(0, bound, WIDE):
            prod = jnp.dot(slhs[0 : 3 * pairs, :], sel[:, b : b + WIDE], preferred_element_type=F32)
            got.append(joined(prod, 0, pairs))
        return got

    def add_received(t, y, v):
        for i, piece in enumerate(pieces(t[...])):
            blhs[i * pairs : (i + 1) * pairs, :] = piece
        for b in range(0, nodes, WIDE):
            s = slice(b, b + WIDE)
            prod = jnp.dot(blhs[...], adj[nodes:, s], preferred_element_type=F32)
            v[:, s] = y[:, s] + joined(prod, 0, pairs)

    def lane_sums(first, second):
        total = None
        for s in tiles(first.shape[1]):
            term = first[:, s] * second[:, s]
            total = term if total is None else total + term
        return total

    def row_of(sums):
        blocks = jnp.concatenate(sums + [jnp.zeros((LANES - pairs * len(sums), LANES), F32)], axis=0)
        return jnp.sum(jnp.transpose(blocks), axis=0, keepdims=True)

    def reduction(stage, peers):
        copies = []
        for d, peer in enumerate(peers, start=1):
            copies.append(
                pltpu.make_async_remote_copy(
                    src_ref=red.at[stage, 0],
                    dst_ref=red.at[stage, d],
                    send_sem=red_send.at[stage, d],
                    recv_sem=red_recv.at[stage, d],
                    device_id={"dom": peer},
                    device_id_type=MESH,
                )
            )
        return copies

    def summed(stage, count):
        terms = [red[stage, d] for d in range(count)]
        while len(terms) > 1:
            terms = [a + b for a, b in zip(terms[0::2], terms[1::2], strict=True)]
        return terms[0]

    def spread_row(row):
        return jnp.transpose(jnp.broadcast_to(row, (LANES, LANES)))

    lhs[6 * pairs :, :] = jnp.zeros((pairs, nodes), BF16)
    for i, piece in enumerate(pieces(cond[...])):
        lhs[6 * pairs + i : 6 * pairs + i + 1, :] = piece
    lhs[6 * pairs + 3 : 6 * pairs + 4, :] = jnp.ones((1, nodes), BF16)
    split_field(cur[...])
    local_operator(cur, y0, True)
    m0 = lane_sums(cur, cur)
    m1 = lane_sums(cur, y0)
    ys = pick_listed(y0, None)

    def pass_on(u, into, t, ys, u_next, out):
        for o in range(links):
            s = slice(o * LANES, (o + 1) * LANES)
            term = wsend[:, s]
            term = jnp.concatenate([term] * (pairs // 8), axis=0) * (u[:, s] - into[o, 0:pairs, :])
            t[:, s] = term
            if u_next is not None:
                inner = s.start % WIDE
                nxt = ys[s.start // WIDE][:, inner : inner + LANES] + term
                u_next[:, s] = nxt
                out[o, :, :] = nxt

    arrive(ex0)
    for o in range(links):
        s = slice(o * LANES, (o + 1) * LANES)
        live = jnp.broadcast_to(send[o : o + 1, :], (8, LANES)) >= 0
        wsend[:, s] = jnp.where(live, half * (wsend[:, s] + in0[o, pairs : pairs + 8, :]), 0.0)
    pass_on(u0, in0, t0, ys, u1, out1)
    ex1 = exchange(1, out1, in1)
    start(ex1)
    m1 = m1 + lane_sums(u0, t0)
    red[0, 0] = row_of([m0, m1])
    near0 = reduction(0, near)
    start(near0)

    add_received(t0, y0, v1)
    split_field(v1[...])
    local_operator(v1, y1, False)
    ys = pick_listed(y1, None)

    arrive(ex1)
    pass_on(u1, in1, t1, ys, u2, out2)
    ex2 = exchange(2, out2, in2)
    start(ex2)
    arrive(near0)
    red[1, 0] = summed(0, group)
    far0 = reduction(1, far)
    start(far0)

    add_received(t1, y1, v2)
    split_field(v2[...])
    local_operator(v2, y2, False)

    arrive(ex2)
    pass_on(u2, in2, t2, None, None, None)
    arrive(far0)
    first_sums = spread_row(summed(1, others))
    m0, m1 = first_sums[0:pairs], first_sums[pairs : 2 * pairs]
    a0 = m0 / m1

    zero = jnp.zeros((pairs, LANES), F32)
    k0, k1, k2, k3 = zero, zero, zero, zero
    for s in tiles(nodes):
        r1 = cur[:, s] - a0 * v1[:, s]
        q1 = v1[:, s] - a0 * v2[:, s]
        k0 = k0 + r1 * r1
        k1 = k1 + r1 * q1
        k2 = k2 + q1 * q1
        k3 = k3 + q1 * (y1[:, s] - a0 * y2[:, s])
    for s in tiles(bound):
        k3 = k3 + (u1[:, s] - a0 * u2[:, s]) * (t1[:, s] - a0 * t2[:, s])
    red[2, 0] = row_of([k0, k1, k2, k3])
    near1 = reduction(2, near)
    start(near1)

    add_received(t2, y2, v3)

    arrive(near1)
    red[3, 0] = summed(2, group)
    far1 = reduction(3, far)
    start(far1)
    arrive(far1)
    sums = spread_row(summed(3, others))
    k0, k1, k2, k3 = (sums[i * pairs : (i + 1) * pairs] for i in range(4))

    b1 = k0 / m0
    a1 = k0 / (k1 - b1 * k0 / a0)
    v1q1 = -(k0 / a0 + k1) / a0
    r2q1 = k1 - a1 * (k2 + b1 * v1q1)
    rr2 = -a1 * r2q1
    b2 = rr2 / k0
    v1q2 = (v1q1 - k2) / a0
    r2q2 = k2 - a1 * (k3 + b1 * v1q2)
    r2ar2 = r2q1 - a1 * (r2q2 - b1 * r2q1 / a0)
    a2 = rr2 / (r2ar2 - b2 * rr2 / a1)

    for s in tiles(nodes):
        w0, w1, w2, w3 = cur[:, s], v1[:, s], v2[:, s], v3[:, s]
        r1 = w0 - a0 * w1
        q1 = w1 - a0 * w2
        q2 = w2 - a0 * w3
        p1 = r1 + b1 * w0
        ap1 = q1 + b1 * w1
        r2 = r1 - a1 * ap1
        ar2 = q1 - a1 * (q2 + b1 * w2)
        p2 = r2 + b2 * p1
        ap2 = ar2 + b2 * ap1
        volt[:, s] = a0 * w0 + a1 * p1 + a2 * p2
        resid[:, s] = r2 - a2 * ap2

    for copies in (ex0, ex1, ex2, near0, far0, near1, far1):
        for copy in copies:
            copy.wait_send()


def solve(parts, group, currents, conductance, ground, ell_cols, send_rows):
    pairs, nodes = currents.shape
    links = send_rows.shape[0]
    bound = links * LANES
    others = parts // group
    most = max(group, others)
    field = pltpu.VMEM((pairs, nodes), F32)
    edge = pltpu.VMEM((pairs, bound), F32)
    vmem = pl.BlockSpec(memory_space=pltpu.VMEM)
    return pl.pallas_call(
        functools.partial(kernel, parts, group),
        out_shape=(jax.ShapeDtypeStruct((pairs, nodes), F32),) * 2,
        in_specs=[vmem] * 5,
        out_specs=(vmem, vmem),
        scratch_shapes=[
            pltpu.VMEM((nodes + bound, nodes), BF16),
            pltpu.VMEM((nodes, bound), BF16),
            field, field, field, field, field, field,
            pltpu.VMEM((1, nodes), F32),
            pltpu.VMEM((7 * pairs, nodes), BF16),
            pltpu.VMEM((3 * pairs, bound), BF16),
            pltpu.VMEM((4 * pairs, nodes), BF16),
            pltpu.VMEM((8, bound), F32),
            edge, edge, edge, edge, edge, edge,
            pltpu.VMEM((links, pairs + 8, LANES), F32),
            pltpu.VMEM((links, pairs, LANES), F32),
            pltpu.VMEM((links, pairs, LANES), F32),
            pltpu.VMEM((links, pairs + 8, LANES), F32),
            pltpu.VMEM((links, pairs, LANES), F32),
            pltpu.VMEM((links, pairs, LANES), F32),
            pltpu.VMEM((4, most, 1, LANES), F32),
            pltpu.SemaphoreType.DMA((3, links)),
            pltpu.SemaphoreType.DMA((3, links)),
            pltpu.SemaphoreType.DMA((4, most)),
            pltpu.SemaphoreType.DMA((4, most)),
        ],
        compiler_params=pltpu.CompilerParams(
            collective_id=0, has_side_effects=True, vmem_limit_bytes=48 * 1024 * 1024
        ),
    )(currents, conductance.reshape(1, nodes), ground.reshape(1, nodes), ell_cols, send_rows)


def solution(mesh):
    parts = mesh.shape["dom"]
    group = 16 if parts >= 256 else 4
    placed = (P(None, "dom"), P("dom"), P("dom"), P(None, "dom"), P("dom", None))
    return jax.shard_map(
        functools.partial(solve, parts, group),
        mesh=mesh,
        in_specs=placed,
        out_specs=(P(None, "dom"), P(None, "dom")),
        check_vma=False,
    )
```

```python
import functools

import jax
import jax.numpy as jnp
from jax import lax
from jax.experimental import pallas as pl
from jax.experimental.pallas import tpu as pltpu
from jax.sharding import PartitionSpec as P

MESH = pl.DeviceIdType.MESH
F32, BF16, I16, I32 = jnp.float32, jnp.bfloat16, jnp.int16, jnp.int32
LANES = 128
WIDE = 256
DIGITS = 8


def pieces(x):
    high = x.astype(BF16)
    rest = x - high.astype(F32)
    mid = rest.astype(BF16)
    low = (rest - mid.astype(F32)).astype(BF16)
    return [high, mid, low]


def joined(y, first, rows):
    return (y[first + 2 * rows : first + 3 * rows] + y[first + rows : first + 2 * rows]) + y[first : first + rows]


def tiles(width):
    return [slice(i, i + LANES) for i in range(0, width, LANES)]


def kernel(
    parts, group, cur_in, cond_in, gnd_in, ell_in, send_in, volt, resid,
    cur, cond, gnd, ell, send, in_sem, adj, sel, v1, v2, v3, y0, y1, y2, diag, lhs, blhs, slhs, wsend, u0, u1, u2, t0, t1, t2,
    out0, out1, out2, in0, in1, in2, red, ex_send, ex_recv, red_send, red_recv,
):
    pairs, nodes = cur.shape
    slots = ell.shape[0]
    links = send.shape[0]
    bound = links * LANES
    reach = links // 2
    offsets = list(range(-reach, 0)) + list(range(1, reach + 1))
    me = lax.axis_index("dom")
    others = parts // group
    mine, place = me // group, me % group

    neighbours = [lax.rem(me + e + parts, parts) for e in offsets]
    near = [mine * group + lax.rem(place + d, group) for d in range(1, group)]
    far = [lax.rem(mine + d, others) * group + place for d in range(1, others)]

    loads = [
        pltpu.make_async_copy(source, target, in_sem.at[i])
        for i, (source, target) in enumerate(
            ((cur_in, cur), (cond_in, cond), (gnd_in, gnd), (ell_in, ell), (send_in, send))
        )
    ]
    loads[4].start()
    loads[0].start()
    for i in range(1, 4):
        loads[i].start()
    barrier = pltpu.get_barrier_semaphore()
    for peer in neighbours + near + far:
        pl.semaphore_signal(barrier, inc=1, device_id={"dom": peer}, device_id_type=MESH)

    ones = jnp.ones((16, LANES), BF16)
    none = jnp.zeros((16, LANES), BF16)
    row_ids = lax.broadcasted_iota(I32, (16, LANES), 0).astype(I16)
    word_ids = lax.broadcasted_iota(I32, (8, LANES), 0)
    no_word = jnp.zeros((8, LANES), I32)
    words = nodes // DIGITS

    def spread(row):
        return jnp.broadcast_to(row, (16, LANES)).astype(I16)

    with jax.named_scope("selbuild"):
        loads[4].wait()
        listed = [spread(send[o : o + 1, :]) for o in range(links)]
        for at in range(0, nodes, 16):
            ids = row_ids + jnp.int16(at)
            for o in range(links):
                sel[o, at : at + 16, :] = jnp.where(listed[o] == ids, ones, none)

    def sel_block(b):
        return jnp.concatenate([sel[b // LANES], sel[b // LANES + 1]], axis=1)

    def picked(y_parts, rows):
        for i, piece in enumerate(y_parts):
            slhs[i * rows : (i + 1) * rows, :] = piece

    loads[0].wait()
    loads[1].wait()
    slhs[...] = jnp.zeros_like(slhs)
    picked(pieces(cur[...]), pairs)
    for i, piece in enumerate(pieces(cond[...])):
        slhs[3 * pairs + i : 3 * pairs + i + 1, :] = piece
    for b in range(0, bound, WIDE):
        y = jnp.dot(slhs[...], sel_block(b), preferred_element_type=F32)
        u0[:, b : b + WIDE] = joined(y, 0, pairs)
        c_part = joined(y, 3 * pairs, 1)
        wsend[:, b : b + WIDE] = jnp.broadcast_to(c_part, (8, WIDE))
    for o in range(links):
        s = slice(o * LANES, (o + 1) * LANES)
        out0[o, 0:pairs, :] = u0[:, s]
        out0[o, pairs : pairs + 8, :] = wsend[:, s]

    def exchange(step, out, into):
        copies = []
        for o in range(links):
            copies.append(
                pltpu.make_async_remote_copy(
                    src_ref=out.at[o],
                    dst_ref=into.at[links - 1 - o],
                    send_sem=ex_send.at[step, o],
                    recv_sem=ex_recv.at[step, links - 1 - o],
                    device_id={"dom": neighbours[o]},
                    device_id_type=MESH,
                )
            )
        return copies

    def start(copies):
        for copy in copies:
            copy.start()

    def arrive(copies):
        for copy in copies:
            copy.wait_recv()

    def build(t, _):
        off = pl.multiple_of(t * LANES, LANES)
        block = ell[:, pl.ds(off, LANES)]
        local = (block >= 0) & (block < nodes)
        wide_g = jnp.where(local, block & (words - 1), -1)
        wide_p = jnp.left_shift(jnp.ones_like(block), jnp.where(local, (block // words) * 4, 0))
        g = [jnp.broadcast_to(wide_g[s : s + 1, :], (8, LANES)) for s in range(slots)]
        p = [jnp.broadcast_to(wide_p[s : s + 1, :], (8, LANES)) for s in range(slots)]
        word = list(p)
        for i in range(slots):
            for j in range(i):
                same = g[i] == g[j]
                word[i] = word[i] + jnp.where(same, p[j], no_word)
                word[j] = word[j] + jnp.where(same, p[i], no_word)
        for h in range(0, words, 64):
            chunk = []
            for q in range(h, h + 64, 8):
                ids = word_ids + q
                acc = no_word
                for s in range(slots):
                    acc = jnp.where(g[s] == ids, word[s], acc)
                chunk.append(acc)
            chunk = jnp.concatenate(chunk, axis=0)
            for r in range(DIGITS):
                last = r == DIGITS - 1
                digit = lax.shift_right_logical(chunk, 4 * r) if last else chunk & (15 << (4 * r))
                adj[t, r * words + h : r * words + h + 64, :] = digit.astype(F32).astype(BF16)
        remote = spread(jnp.max(block, axis=0, keepdims=True))
        for at in range(nodes, nodes + bound, 16):
            adj[t, at : at + 16, :] = jnp.where(remote == row_ids + jnp.int16(at), ones, none)
        return 0

    def adj_block(b, first, last):
        return jnp.concatenate([adj[b // LANES, first:last, :], adj[b // LANES + 1, first:last, :]], axis=1)

    def scale_of(r):
        return 1.0 if r == DIGITS - 1 else 16.0**-r

    def split_field(v):
        for r in range(DIGITS):
            s = slice(r * words, (r + 1) * words)
            part = v[:, s] * scale_of(r)
            for i, piece in enumerate(pieces(part)):
                lhs[i * pairs : (i + 1) * pairs, s] = piece
            for i, piece in enumerate(pieces(part * cond[:, s])):
                lhs[(3 + i) * pairs : (4 + i) * pairs, s] = piece

    half = 0.5
    with jax.named_scope("adj_a"):
        loads[3].wait()
        lax.fori_loop(0, nodes // LANES // 2, build, 0)
    with jax.named_scope("barwait"):
        pl.semaphore_wait(barrier, len(neighbours) + len(near) + len(far))
    ex0 = exchange(0, out0, in0)
    start(ex0)
    with jax.named_scope("adj_b"):
        lax.fori_loop(nodes // LANES // 2, nodes // LANES, build, 0)

    def local_operator(v, y, first):
        rows = 7 * pairs if first else 6 * pairs
        for b in range(0, nodes, WIDE):
            s = slice(b, b + WIDE)
            prod = jnp.dot(lhs[0:rows, :], adj_block(b, 0, nodes), preferred_element_type=F32)
            c = cond[:, s]
            if first:
                extra = prod[6 * pairs :]
                around = joined(extra, 0, 1)
                diag[:, s] = gnd[:, s] + half * (c * extra[3:4] + around)
            y[:, s] = diag[:, s] * v[:, s] - half * (c * joined(prod, 0, pairs) + joined(prod, 3 * pairs, pairs))

    def pick_listed(y, start_with):
        picked(pieces(y[...]), pairs)
        got = []
        for b in range(0, bound, WIDE):
            prod = jnp.dot(slhs[0 : 3 * pairs, :], sel_block(b), preferred_element_type=F32)
            got.append(joined(prod, 0, pairs))
        return got

    def add_received(t, y, v):
        for i, piece in enumerate(pieces(t[...])):
            blhs[i * pairs : (i + 1) * pairs, :] = piece
        for b in range(0, nodes, WIDE):
            s = slice(b, b + WIDE)
            prod = jnp.dot(blhs[...], adj_block(b, nodes, nodes + bound), preferred_element_type=F32)
            v[:, s] = y[:, s] + joined(prod, 0, pairs)

    def lane_sums(first, second):
        total = None
        for s in tiles(first.shape[1]):
            term = first[:, s] * second[:, s]
            total = term if total is None else total + term
        return total

    def row_of(sums):
        blocks = jnp.concatenate(sums + [jnp.zeros((LANES - pairs * len(sums), LANES), F32)], axis=0)
        return jnp.sum(jnp.transpose(blocks), axis=0, keepdims=True)

    def reduction(stage, peers):
        copies = []
        for d, peer in enumerate(peers, start=1):
            copies.append(
                pltpu.make_async_remote_copy(
                    src_ref=red.at[stage, 0],
                    dst_ref=red.at[stage, d],
                    send_sem=red_send.at[stage, d],
                    recv_sem=red_recv.at[stage, d],
                    device_id={"dom": peer},
                    device_id_type=MESH,
                )
            )
        return copies

    def summed(stage, count):
        terms = [red[stage, d] for d in range(count)]
        while len(terms) > 1:
            terms = [a + b for a, b in zip(terms[0::2], terms[1::2], strict=True)]
        return terms[0]

    def spread_row(row):
        return jnp.transpose(jnp.broadcast_to(row, (LANES, LANES)))

    lhs[6 * pairs :, :] = jnp.zeros((pairs, nodes), BF16)
    loads[2].wait()
    for r in range(DIGITS):
        s = slice(r * words, (r + 1) * words)
        for i, piece in enumerate(pieces(cond[:, s] * scale_of(r))):
            lhs[6 * pairs + i : 6 * pairs + i + 1, s] = piece
        lhs[6 * pairs + 3 : 6 * pairs + 4, s] = jnp.full((1, words), scale_of(r), BF16)
    split_field(cur)
    local_operator(cur, y0, True)
    m0 = lane_sums(cur, cur)
    m1 = lane_sums(cur, y0)
    ys = pick_listed(y0, None)

    def pass_on(u, into, t, ys, u_next, out):
        for o in range(links):
            s = slice(o * LANES, (o + 1) * LANES)
            term = wsend[:, s]
            term = jnp.concatenate([term] * (pairs // 8), axis=0) * (u[:, s] - into[o, 0:pairs, :])
            t[:, s] = term
            if u_next is not None:
                inner = s.start % WIDE
                nxt = ys[s.start // WIDE][:, inner : inner + LANES] + term
                u_next[:, s] = nxt
                out[o, :, :] = nxt

    arrive(ex0)
    for o in range(links):
        s = slice(o * LANES, (o + 1) * LANES)
        live = jnp.broadcast_to(send[o : o + 1, :], (8, LANES)) >= 0
        wsend[:, s] = jnp.where(live, half * (wsend[:, s] + in0[o, pairs : pairs + 8, :]), 0.0)
    pass_on(u0, in0, t0, ys, u1, out1)
    ex1 = exchange(1, out1, in1)
    start(ex1)
    m1 = m1 + lane_sums(u0, t0)
    red[0, 0] = row_of([m0, m1])
    near0 = reduction(0, near)
    start(near0)

    add_received(t0, y0, v1)
    split_field(v1)
    local_operator(v1, y1, False)
    ys = pick_listed(y1, None)

    arrive(ex1)
    pass_on(u1, in1, t1, ys, u2, out2)
    ex2 = exchange(2, out2, in2)
    start(ex2)
    arrive(near0)
    red[1, 0] = summed(0, group)
    far0 = reduction(1, far)
    start(far0)

    add_received(t1, y1, v2)
    split_field(v2)
    local_operator(v2, y2, False)

    arrive(ex2)
    pass_on(u2, in2, t2, None, None, None)
    arrive(far0)
    first_sums = spread_row(summed(1, others))
    m0, m1 = first_sums[0:pairs], first_sums[pairs : 2 * pairs]
    a0 = m0 / m1

    zero = jnp.zeros((pairs, LANES), F32)
    k0, k1, k2, k3 = zero, zero, zero, zero
    for s in tiles(nodes):
        r1 = cur[:, s] - a0 * v1[:, s]
        q1 = v1[:, s] - a0 * v2[:, s]
        k0 = k0 + r1 * r1
        k1 = k1 + r1 * q1
        k2 = k2 + q1 * q1
        k3 = k3 + q1 * (y1[:, s] - a0 * y2[:, s])
    for s in tiles(bound):
        k3 = k3 + (u1[:, s] - a0 * u2[:, s]) * (t1[:, s] - a0 * t2[:, s])
    red[2, 0] = row_of([k0, k1, k2, k3])
    near1 = reduction(2, near)
    start(near1)

    add_received(t2, y2, v3)

    arrive(near1)
    red[3, 0] = summed(2, group)
    far1 = reduction(3, far)
    start(far1)
    arrive(far1)
    sums = spread_row(summed(3, others))
    k0, k1, k2, k3 = (sums[i * pairs : (i + 1) * pairs] for i in range(4))

    b1 = k0 / m0
    a1 = k0 / (k1 - b1 * k0 / a0)
    v1q1 = -(k0 / a0 + k1) / a0
    r2q1 = k1 - a1 * (k2 + b1 * v1q1)
    rr2 = -a1 * r2q1
    b2 = rr2 / k0
    v1q2 = (v1q1 - k2) / a0
    r2q2 = k2 - a1 * (k3 + b1 * v1q2)
    r2ar2 = r2q1 - a1 * (r2q2 - b1 * r2q1 / a0)
    a2 = rr2 / (r2ar2 - b2 * rr2 / a1)

    for s in tiles(nodes):
        w0, w1, w2, w3 = cur[:, s], v1[:, s], v2[:, s], v3[:, s]
        r1 = w0 - a0 * w1
        q1 = w1 - a0 * w2
        q2 = w2 - a0 * w3
        p1 = r1 + b1 * w0
        ap1 = q1 + b1 * w1
        r2 = r1 - a1 * ap1
        ar2 = q1 - a1 * (q2 + b1 * w2)
        p2 = r2 + b2 * p1
        ap2 = ar2 + b2 * ap1
        volt[:, s] = a0 * w0 + a1 * p1 + a2 * p2
        resid[:, s] = r2 - a2 * ap2

    for copies in (ex0, ex1, ex2, near0, far0, near1, far1):
        for copy in copies:
            copy.wait_send()


def write_out(volt, resid, volt_out, resid_out, sems):
    copies = [pltpu.make_async_copy(volt, volt_out, sems.at[0]), pltpu.make_async_copy(resid, resid_out, sems.at[1])]
    for copy in copies:
        copy.start()
    for copy in copies:
        copy.wait()


def solve(parts, group, currents, conductance, ground, ell_cols, send_rows):
    pairs, nodes = currents.shape
    links = send_rows.shape[0]
    bound = links * LANES
    others = parts // group
    most = max(group, others)
    field = pltpu.VMEM((pairs, nodes), F32)
    edge = pltpu.VMEM((pairs, bound), F32)
    vmem = pl.BlockSpec(memory_space=pltpu.VMEM)
    volt, resid = pl.pallas_call(
        functools.partial(kernel, parts, group),
        out_shape=(jax.ShapeDtypeStruct((pairs, nodes), F32),) * 2,
        in_specs=[pl.BlockSpec(memory_space=pltpu.HBM)] * 5,
        out_specs=(vmem, vmem),
        scratch_shapes=[
            field,
            pltpu.VMEM((1, nodes), F32),
            pltpu.VMEM((1, nodes), F32),
            pltpu.VMEM(ell_cols.shape, I32),
            pltpu.VMEM(send_rows.shape, I32),
            pltpu.SemaphoreType.DMA((5,)),
            pltpu.VMEM((nodes // LANES, nodes + bound, LANES), BF16),
            pltpu.VMEM((links, nodes, LANES), BF16),
            field, field, field, field, field, field,
            pltpu.VMEM((1, nodes), F32),
            pltpu.VMEM((7 * pairs, nodes), BF16),
            pltpu.VMEM((3 * pairs, bound), BF16),
            pltpu.VMEM((4 * pairs, nodes), BF16),
            pltpu.VMEM((8, bound), F32),
            edge, edge, edge, edge, edge, edge,
            pltpu.VMEM((links, pairs + 8, LANES), F32),
            pltpu.VMEM((links, pairs, LANES), F32),
            pltpu.VMEM((links, pairs, LANES), F32),
            pltpu.VMEM((links, pairs + 8, LANES), F32),
            pltpu.VMEM((links, pairs, LANES), F32),
            pltpu.VMEM((links, pairs, LANES), F32),
            pltpu.VMEM((4, most, 1, LANES), F32),
            pltpu.SemaphoreType.DMA((3, links)),
            pltpu.SemaphoreType.DMA((3, links)),
            pltpu.SemaphoreType.DMA((4, most)),
            pltpu.SemaphoreType.DMA((4, most)),
        ],
        compiler_params=pltpu.CompilerParams(
            collective_id=0, has_side_effects=True, vmem_limit_bytes=48 * 1024 * 1024
        ),
    )(*(pltpu.with_memory_space_constraint(x, pltpu.HBM) for x in (currents, conductance.reshape(1, nodes), ground.reshape(1, nodes), ell_cols, send_rows)))
    return pl.pallas_call(
        write_out,
        out_shape=(jax.ShapeDtypeStruct((pairs, nodes), F32),) * 2,
        in_specs=[vmem] * 2,
        out_specs=(pl.BlockSpec(memory_space=pltpu.HBM),) * 2,
        scratch_shapes=[pltpu.SemaphoreType.DMA((2,))],
        compiler_params=pltpu.CompilerParams(vmem_limit_bytes=1 << 20),
    )(volt, resid)


def solution(mesh):
    parts = mesh.shape["dom"]
    group = 16 if parts >= 256 else 4
    placed = (P(None, "dom"), P("dom"), P("dom"), P(None, "dom"), P("dom", None))
    return jax.shard_map(
        functools.partial(solve, parts, group),
        mesh=mesh,
        in_specs=placed,
        out_specs=(P(None, "dom"), P(None, "dom")),
        check_vma=False,
    )
```

```python
import functools

import jax
import jax.numpy as jnp
from jax import lax
from jax.experimental import pallas as pl
from jax.experimental.pallas import tpu as pltpu
from jax.sharding import PartitionSpec as P

MESH = pl.DeviceIdType.MESH
F32, BF16, I16, I32 = jnp.float32, jnp.bfloat16, jnp.int16, jnp.int32
LANES = 128
WIDE = 256
DIGITS = 8


def pieces(x):
    high = x.astype(BF16)
    rest = x - high.astype(F32)
    mid = rest.astype(BF16)
    low = (rest - mid.astype(F32)).astype(BF16)
    return [high, mid, low]


def joined(y, first, rows):
    return (y[first + 2 * rows : first + 3 * rows] + y[first + rows : first + 2 * rows]) + y[first : first + rows]


def tiles(width):
    return [slice(i, i + LANES) for i in range(0, width, LANES)]


def kernel(
    parts, group, cur_in, cond_in, gnd_in, ell_in, send_in, volt, resid,
    cur, cond, gnd, ell, send, in_sem, adj, sel, v1, v2, v3, y0, y1, y2, diag, lhs, blhs, slhs, wsend, u0, u1, u2, t0, t1, t2,
    out0, out1, out2, in0, in1, in2, red, ex_send, ex_recv, red_send, red_recv,
):
    pairs, nodes = cur.shape
    slots = ell.shape[0]
    links = send.shape[0]
    bound = links * LANES
    reach = links // 2
    offsets = list(range(-reach, 0)) + list(range(1, reach + 1))
    me = lax.axis_index("dom")
    others = parts // group
    mine, place = me // group, me % group

    assert reach == 3
    neighbours, landing = [], []
    for o, e in enumerate(offsets):
        d = abs(e)
        edge = me if e < 0 else parts - 1 - me
        spare = jnp.where(edge == 0, 1 if d < 3 else 2, 0)
        spare_d = jnp.where(edge == 0, min(d + 1, 3), jnp.where(edge == 1, d - 1, 3))
        inside = edge >= d
        spare_peer = spare if e < 0 else parts - 1 - spare
        spare_slot = reach - spare_d if e < 0 else reach - 1 + spare_d
        neighbours.append(jnp.where(inside, me + e, spare_peer))
        landing.append(jnp.where(inside, links - 1 - o, spare_slot))
    near = [mine * group + lax.rem(place + d, group) for d in range(1, group)]
    far = [lax.rem(mine + d, others) * group + place for d in range(1, others)]

    barrier = pltpu.get_barrier_semaphore()
    for peer in neighbours + near + far:
        pl.semaphore_signal(barrier, inc=1, device_id={"dom": peer}, device_id_type=MESH)
    loads = [
        pltpu.make_async_copy(source, target, in_sem.at[i])
        for i, (source, target) in enumerate(
            ((cur_in, cur), (cond_in, cond), (gnd_in, gnd), (ell_in, ell), (send_in, send))
        )
    ]
    loads[4].start()
    loads[0].start()
    for i in range(1, 4):
        loads[i].start()

    ones = jnp.ones((16, LANES), BF16)
    none = jnp.zeros((16, LANES), BF16)
    row_ids = lax.broadcasted_iota(I32, (16, LANES), 0).astype(I16)
    word_ids = lax.broadcasted_iota(I32, (8, LANES), 0)
    no_word = jnp.zeros((8, LANES), I32)
    words = nodes // DIGITS

    def spread(row):
        return jnp.broadcast_to(row, (16, LANES)).astype(I16)

    with jax.named_scope("selbuild"):
        loads[4].wait()
        listed = [spread(send[o : o + 1, :]) for o in range(links)]
        for at in range(0, nodes, 16):
            ids = row_ids + jnp.int16(at)
            for o in range(links):
                sel[o, at : at + 16, :] = jnp.where(listed[o] == ids, ones, none)

    def sel_block(b):
        return jnp.concatenate([sel[b // LANES], sel[b // LANES + 1]], axis=1)

    def picked(y_parts, rows):
        for i, piece in enumerate(y_parts):
            slhs[i * rows : (i + 1) * rows, :] = piece

    loads[0].wait()
    loads[1].wait()
    slhs[...] = jnp.zeros_like(slhs)
    picked(pieces(cur[...]), pairs)
    for i, piece in enumerate(pieces(cond[...])):
        slhs[3 * pairs + i : 3 * pairs + i + 1, :] = piece
    for b in range(0, bound, WIDE):
        y = jnp.dot(slhs[...], sel_block(b), preferred_element_type=F32)
        u0[:, b : b + WIDE] = joined(y, 0, pairs)
        c_part = joined(y, 3 * pairs, 1)
        wsend[:, b : b + WIDE] = jnp.broadcast_to(c_part, (8, WIDE))
    for o in range(links):
        s = slice(o * LANES, (o + 1) * LANES)
        out0[o, 0:pairs, :] = u0[:, s]
        out0[o, pairs : pairs + 8, :] = wsend[:, s]

    def exchange(step, out, into):
        for o in range(links):
            pltpu.make_async_remote_copy(
                src_ref=out.at[o],
                dst_ref=into.at[landing[o]],
                send_sem=ex_send.at[step],
                recv_sem=ex_recv.at[step],
                device_id={"dom": neighbours[o]},
                device_id_type=MESH,
            ).start()
        return pltpu.make_async_remote_copy(
            src_ref=out, dst_ref=into, send_sem=ex_send.at[step], recv_sem=ex_recv.at[step],
            device_id={"dom": neighbours[0]}, device_id_type=MESH,
        )

    def build(t, _):
        off = pl.multiple_of(t * LANES, LANES)
        block = ell[:, pl.ds(off, LANES)]
        local = (block >= 0) & (block < nodes)
        wide_g = jnp.where(local, block & (words - 1), -1)
        wide_p = jnp.left_shift(jnp.ones_like(block), jnp.where(local, (block // words) * 4, 0))
        g = [jnp.broadcast_to(wide_g[s : s + 1, :], (8, LANES)) for s in range(slots)]
        p = [jnp.broadcast_to(wide_p[s : s + 1, :], (8, LANES)) for s in range(slots)]
        word = list(p)
        for i in range(slots):
            for j in range(i):
                same = g[i] == g[j]
                word[i] = word[i] + jnp.where(same, p[j], no_word)
                word[j] = word[j] + jnp.where(same, p[i], no_word)
        for h in range(0, words, 64):
            chunk = []
            for q in range(h, h + 64, 8):
                ids = word_ids + q
                acc = no_word
                for s in range(slots):
                    acc = jnp.where(g[s] == ids, word[s], acc)
                chunk.append(acc)
            chunk = jnp.concatenate(chunk, axis=0)
            for r in range(DIGITS):
                last = r == DIGITS - 1
                digit = lax.shift_right_logical(chunk, 4 * r) if last else chunk & (15 << (4 * r))
                adj[t, r * words + h : r * words + h + 64, :] = digit.astype(F32).astype(BF16)
        remote = spread(jnp.max(block, axis=0, keepdims=True))
        for at in range(nodes, nodes + bound, 16):
            adj[t, at : at + 16, :] = jnp.where(remote == row_ids + jnp.int16(at), ones, none)
        return 0

    def adj_block(b, first, last):
        return jnp.concatenate([adj[b // LANES, first:last, :], adj[b // LANES + 1, first:last, :]], axis=1)

    def scale_of(r):
        return 1.0 if r == DIGITS - 1 else 16.0**-r

    def split_field(v):
        for r in range(DIGITS):
            s = slice(r * words, (r + 1) * words)
            part = v[:, s] * scale_of(r)
            for i, piece in enumerate(pieces(part)):
                lhs[i * pairs : (i + 1) * pairs, s] = piece
            for i, piece in enumerate(pieces(part * cond[:, s])):
                lhs[(3 + i) * pairs : (4 + i) * pairs, s] = piece

    half = 0.5
    with jax.named_scope("adj_a"):
        loads[3].wait()
        ahead = jnp.where(place < group // 2, nodes // LANES, nodes // LANES // 4)
        lax.fori_loop(0, ahead, build, 0)
    with jax.named_scope("barwait"):
        pl.semaphore_wait(barrier, len(neighbours) + len(near) + len(far))
    ex0 = exchange(0, out0, in0)
    with jax.named_scope("adj_b"):
        lax.fori_loop(ahead, nodes // LANES, build, 0)

    def local_operator(v, y, first):
        rows = 7 * pairs if first else 6 * pairs
        for b in range(0, nodes, WIDE):
            s = slice(b, b + WIDE)
            prod = jnp.dot(lhs[0:rows, :], adj_block(b, 0, nodes), preferred_element_type=F32)
            c = cond[:, s]
            if first:
                extra = prod[6 * pairs :]
                around = joined(extra, 0, 1)
                diag[:, s] = gnd[:, s] + half * (c * extra[3:4] + around)
            y[:, s] = diag[:, s] * v[:, s] - half * (c * joined(prod, 0, pairs) + joined(prod, 3 * pairs, pairs))

    def pick_listed(y, start_with):
        picked(pieces(y[...]), pairs)
        got = []
        for b in range(0, bound, WIDE):
            prod = jnp.dot(slhs[0 : 3 * pairs, :], sel_block(b), preferred_element_type=F32)
            got.append(joined(prod, 0, pairs))
        return got

    def add_received(t, y, v):
        for i, piece in enumerate(pieces(t[...])):
            blhs[i * pairs : (i + 1) * pairs, :] = piece
        for b in range(0, nodes, WIDE):
            s = slice(b, b + WIDE)
            prod = jnp.dot(blhs[...], adj_block(b, nodes, nodes + bound), preferred_element_type=F32)
            v[:, s] = y[:, s] + joined(prod, 0, pairs)

    def lane_sums(first, second):
        total = None
        for s in tiles(first.shape[1]):
            term = first[:, s] * second[:, s]
            total = term if total is None else total + term
        return total

    def row_of(sums):
        blocks = jnp.concatenate(sums + [jnp.zeros((LANES - pairs * len(sums), LANES), F32)], axis=0)
        return jnp.sum(jnp.transpose(blocks), axis=0, keepdims=True)

    def reduction(stage, peers):
        for d, peer in enumerate(peers, start=1):
            pltpu.make_async_remote_copy(
                src_ref=red.at[stage, 0],
                dst_ref=red.at[stage, d],
                send_sem=red_send.at[stage],
                recv_sem=red_recv.at[stage],
                device_id={"dom": peer},
                device_id_type=MESH,
            ).start()
        slots_used = red.at[stage, 1 : len(peers) + 1]
        return pltpu.make_async_remote_copy(
            src_ref=slots_used, dst_ref=slots_used, send_sem=red_send.at[stage], recv_sem=red_recv.at[stage],
            device_id={"dom": peers[0]}, device_id_type=MESH,
        )

    def summed(stage, count):
        terms = [red[stage, d] for d in range(count)]
        while len(terms) > 1:
            terms = [a + b for a, b in zip(terms[0::2], terms[1::2], strict=True)]
        return terms[0]

    def spread_row(row):
        return jnp.transpose(jnp.broadcast_to(row, (LANES, LANES)))

    lhs[6 * pairs :, :] = jnp.zeros((pairs, nodes), BF16)
    loads[2].wait()
    for r in range(DIGITS):
        s = slice(r * words, (r + 1) * words)
        for i, piece in enumerate(pieces(cond[:, s] * scale_of(r))):
            lhs[6 * pairs + i : 6 * pairs + i + 1, s] = piece
        lhs[6 * pairs + 3 : 6 * pairs + 4, s] = jnp.full((1, words), scale_of(r), BF16)
    split_field(cur)
    local_operator(cur, y0, True)
    m0 = lane_sums(cur, cur)
    m1 = lane_sums(cur, y0)
    ys = pick_listed(y0, None)

    def pass_on(u, into, t, ys, u_next, out):
        for o in range(links):
            s = slice(o * LANES, (o + 1) * LANES)
            term = wsend[:, s]
            term = jnp.concatenate([term] * (pairs // 8), axis=0) * (u[:, s] - into[o, 0:pairs, :])
            t[:, s] = term
            if u_next is not None:
                inner = s.start % WIDE
                nxt = ys[s.start // WIDE][:, inner : inner + LANES] + term
                u_next[:, s] = nxt
                out[o, :, :] = nxt

    ex0.wait_recv()
    for o in range(links):
        s = slice(o * LANES, (o + 1) * LANES)
        live = jnp.broadcast_to(send[o : o + 1, :], (8, LANES)) >= 0
        wsend[:, s] = jnp.where(live, half * (wsend[:, s] + in0[o, pairs : pairs + 8, :]), 0.0)
    pass_on(u0, in0, t0, ys, u1, out1)
    ex1 = exchange(1, out1, in1)
    m1 = m1 + lane_sums(u0, t0)
    red[0, 0] = row_of([m0, m1])
    near0 = reduction(0, near)

    add_received(t0, y0, v1)
    split_field(v1)
    local_operator(v1, y1, False)
    ys = pick_listed(y1, None)

    ex1.wait_recv()
    pass_on(u1, in1, t1, ys, u2, out2)
    ex2 = exchange(2, out2, in2)
    near0.wait_recv()
    red[1, 0] = summed(0, group)
    far0 = reduction(1, far)

    add_received(t1, y1, v2)
    split_field(v2)
    local_operator(v2, y2, False)

    ex2.wait_recv()
    pass_on(u2, in2, t2, None, None, None)
    far0.wait_recv()
    first_sums = spread_row(summed(1, others))
    m0, m1 = first_sums[0:pairs], first_sums[pairs : 2 * pairs]
    a0 = m0 / m1

    zero = jnp.zeros((pairs, LANES), F32)
    k0, k1, k2, k3 = zero, zero, zero, zero
    for s in tiles(nodes):
        r1 = cur[:, s] - a0 * v1[:, s]
        q1 = v1[:, s] - a0 * v2[:, s]
        k0 = k0 + r1 * r1
        k1 = k1 + r1 * q1
        k2 = k2 + q1 * q1
        k3 = k3 + q1 * (y1[:, s] - a0 * y2[:, s])
    for s in tiles(bound):
        k3 = k3 + (u1[:, s] - a0 * u2[:, s]) * (t1[:, s] - a0 * t2[:, s])
    red[2, 0] = row_of([k0, k1, k2, k3])
    near1 = reduction(2, near)

    add_received(t2, y2, v3)

    near1.wait_recv()
    red[3, 0] = summed(2, group)
    far1 = reduction(3, far)
    far1.wait_recv()
    sums = spread_row(summed(3, others))
    k0, k1, k2, k3 = (sums[i * pairs : (i + 1) * pairs] for i in range(4))

    b1 = k0 / m0
    a1 = k0 / (k1 - b1 * k0 / a0)
    v1q1 = -(k0 / a0 + k1) / a0
    r2q1 = k1 - a1 * (k2 + b1 * v1q1)
    rr2 = -a1 * r2q1
    b2 = rr2 / k0
    v1q2 = (v1q1 - k2) / a0
    r2q2 = k2 - a1 * (k3 + b1 * v1q2)
    r2ar2 = r2q1 - a1 * (r2q2 - b1 * r2q1 / a0)
    a2 = rr2 / (r2ar2 - b2 * rr2 / a1)

    for s in tiles(nodes):
        w0, w1, w2, w3 = cur[:, s], v1[:, s], v2[:, s], v3[:, s]
        r1 = w0 - a0 * w1
        q1 = w1 - a0 * w2
        q2 = w2 - a0 * w3
        p1 = r1 + b1 * w0
        ap1 = q1 + b1 * w1
        r2 = r1 - a1 * ap1
        ar2 = q1 - a1 * (q2 + b1 * w2)
        p2 = r2 + b2 * p1
        ap2 = ar2 + b2 * ap1
        volt[:, s] = a0 * w0 + a1 * p1 + a2 * p2
        resid[:, s] = r2 - a2 * ap2

    for copies in (ex0, ex1, ex2, near0, far0, near1, far1):
        copies.wait_send()


def write_out(volt, resid, volt_out, resid_out, sems):
    copies = [pltpu.make_async_copy(volt, volt_out, sems.at[0]), pltpu.make_async_copy(resid, resid_out, sems.at[1])]
    for copy in copies:
        copy.start()
    for copy in copies:
        copy.wait()


def solve(parts, group, currents, conductance, ground, ell_cols, send_rows):
    pairs, nodes = currents.shape
    links = send_rows.shape[0]
    bound = links * LANES
    others = parts // group
    most = max(group, others)
    field = pltpu.VMEM((pairs, nodes), F32)
    edge = pltpu.VMEM((pairs, bound), F32)
    vmem = pl.BlockSpec(memory_space=pltpu.VMEM)
    volt, resid = pl.pallas_call(
        functools.partial(kernel, parts, group),
        out_shape=(jax.ShapeDtypeStruct((pairs, nodes), F32),) * 2,
        in_specs=[pl.BlockSpec(memory_space=pltpu.HBM)] * 5,
        out_specs=(vmem, vmem),
        scratch_shapes=[
            field,
            pltpu.VMEM((1, nodes), F32),
            pltpu.VMEM((1, nodes), F32),
            pltpu.VMEM(ell_cols.shape, I32),
            pltpu.VMEM(send_rows.shape, I32),
            pltpu.SemaphoreType.DMA((5,)),
            pltpu.VMEM((nodes // LANES, nodes + bound, LANES), BF16),
            pltpu.VMEM((links, nodes, LANES), BF16),
            field, field, field, field, field, field,
            pltpu.VMEM((1, nodes), F32),
            pltpu.VMEM((7 * pairs, nodes), BF16),
            pltpu.VMEM((3 * pairs, bound), BF16),
            pltpu.VMEM((4 * pairs, nodes), BF16),
            pltpu.VMEM((8, bound), F32),
            edge, edge, edge, edge, edge, edge,
            pltpu.VMEM((links, pairs + 8, LANES), F32),
            pltpu.VMEM((links, pairs, LANES), F32),
            pltpu.VMEM((links, pairs, LANES), F32),
            pltpu.VMEM((links, pairs + 8, LANES), F32),
            pltpu.VMEM((links, pairs, LANES), F32),
            pltpu.VMEM((links, pairs, LANES), F32),
            pltpu.VMEM((4, most, 1, LANES), F32),
            pltpu.SemaphoreType.DMA((3,)),
            pltpu.SemaphoreType.DMA((3,)),
            pltpu.SemaphoreType.DMA((4,)),
            pltpu.SemaphoreType.DMA((4,)),
        ],
        compiler_params=pltpu.CompilerParams(
            collective_id=0, has_side_effects=True, vmem_limit_bytes=48 * 1024 * 1024
        ),
    )(*(pltpu.with_memory_space_constraint(x, pltpu.HBM) for x in (currents, conductance.reshape(1, nodes), ground.reshape(1, nodes), ell_cols, send_rows)))
    return pl.pallas_call(
        write_out,
        out_shape=(jax.ShapeDtypeStruct((pairs, nodes), F32),) * 2,
        in_specs=[vmem] * 2,
        out_specs=(pl.BlockSpec(memory_space=pltpu.HBM),) * 2,
        scratch_shapes=[pltpu.SemaphoreType.DMA((2,))],
        compiler_params=pltpu.CompilerParams(vmem_limit_bytes=1 << 20),
    )(volt, resid)


def solution(mesh):
    parts = mesh.shape["dom"]
    group = 16 if parts >= 256 else 4
    placed = (P(None, "dom"), P("dom"), P("dom"), P(None, "dom"), P("dom", None))
    return jax.shard_map(
        functools.partial(solve, parts, group),
        mesh=mesh,
        in_specs=placed,
        out_specs=(P(None, "dom"), P(None, "dom")),
        check_vma=False,
    )
```

```python
import functools

import jax
import jax.numpy as jnp
from jax import lax
from jax.experimental import pallas as pl
from jax.experimental.pallas import tpu as pltpu
from jax.sharding import PartitionSpec as P

MESH = pl.DeviceIdType.MESH
F32, BF16, I32 = jnp.float32, jnp.bfloat16, jnp.int32
LANES = 128
WIDE = 256
DIGITS = 8


def pieces(x):
    high = x.astype(BF16)
    rest = x - high.astype(F32)
    mid = rest.astype(BF16)
    low = (rest - mid.astype(F32)).astype(BF16)
    return [high, mid, low]


def joined(y, first, rows):
    return (y[first + 2 * rows : first + 3 * rows] + y[first + rows : first + 2 * rows]) + y[first : first + rows]


def tiles(width):
    return [slice(i, i + LANES) for i in range(0, width, LANES)]


def kernel(
    parts, group, cur_in, cond_in, gnd_in, ell_in, send_in, volt, resid,
    cur, cond, gnd, ell, send, in_sem, adj, from_slot, v1, v2, v3, y0, y1, y2, diag, lhs, wsend, u0, u1, u2, t0, t1, t2,
    out0, out1, out2, in0, in1, in2, red, ex_send, ex_recv, red_send, red_recv,
):
    pairs, nodes = cur.shape
    slots = ell.shape[0]
    links = send.shape[0]
    bound = links * LANES
    reach = links // 2
    offsets = list(range(-reach, 0)) + list(range(1, reach + 1))
    me = lax.axis_index("dom")
    others = parts // group
    mine, place = me // group, me % group

    assert reach == 3
    neighbours, landing = [], []
    for o, e in enumerate(offsets):
        d = abs(e)
        edge = me if e < 0 else parts - 1 - me
        spare = jnp.where(edge == 0, 1 if d < 3 else 2, 0)
        spare_d = jnp.where(edge == 0, min(d + 1, 3), jnp.where(edge == 1, d - 1, 3))
        inside = edge >= d
        spare_peer = spare if e < 0 else parts - 1 - spare
        spare_slot = reach - spare_d if e < 0 else reach - 1 + spare_d
        neighbours.append(jnp.where(inside, me + e, spare_peer))
        landing.append(jnp.where(inside, links - 1 - o, spare_slot))
    near = [mine * group + lax.rem(place + d, group) for d in range(1, group)]
    far = [lax.rem(mine + d, others) * group + place for d in range(1, others)]

    loads = [
        pltpu.make_async_copy(source, target, in_sem.at[i])
        for i, (source, target) in enumerate(
            ((cur_in, cur), (cond_in, cond), (gnd_in, gnd), (ell_in, ell), (send_in, send))
        )
    ]
    loads[4].start()
    loads[0].start()
    for i in range(1, 4):
        loads[i].start()

    barrier = pltpu.get_barrier_semaphore()
    for peer in neighbours + near + far:
        pl.semaphore_signal(barrier, inc=1, device_id={"dom": peer}, device_id_type=MESH)
    word_ids = lax.broadcasted_iota(I32, (8, LANES), 0)
    no_word = jnp.zeros((8, LANES), I32)
    words = nodes // DIGITS

    def taken(x, lane):
        return jnp.take_along_axis(x, lane, axis=1, mode="promise_in_bounds")

    def picked(source, rows):
        found = []
        for o in range(links):
            node = jnp.broadcast_to(send[o : o + 1, :], (8, LANES))
            lane, tile = node & (LANES - 1), lax.shift_right_arithmetic(node, 7)
            parts_found = [jnp.zeros((8, LANES), F32)] * (rows // 8)
            for k, s in enumerate(tiles(nodes)):
                here = tile == k
                for i in range(rows // 8):
                    parts_found[i] = jnp.where(here, taken(source(i, s), lane), parts_found[i])
            found.append(jnp.concatenate(parts_found, axis=0))
        return found

    def field_rows(field):
        return lambda i, s: field[i * 8 : i * 8 + 8, s]

    with jax.named_scope("pick_cur"):
        loads[4].wait()
        loads[0].wait()
        loads[1].wait()
        for o, (u, c) in enumerate(
            zip(
                picked(field_rows(cur), pairs),
                picked(lambda i, s: jnp.broadcast_to(cond[:, s], (8, LANES)), 8),
                strict=True,
            )
        ):
            s = slice(o * LANES, (o + 1) * LANES)
            u0[:, s] = u
            wsend[:, s] = c
            out0[o, 0:pairs, :] = u
            out0[o, pairs : pairs + 8, :] = c

    def exchange(step, out, into):
        for o in range(links):
            pltpu.make_async_remote_copy(
                src_ref=out.at[o],
                dst_ref=into.at[landing[o]],
                send_sem=ex_send.at[step],
                recv_sem=ex_recv.at[step],
                device_id={"dom": neighbours[o]},
                device_id_type=MESH,
            ).start()
        return pltpu.make_async_remote_copy(
            src_ref=out, dst_ref=into, send_sem=ex_send.at[step], recv_sem=ex_recv.at[step],
            device_id={"dom": neighbours[0]}, device_id_type=MESH,
        )

    def build(t, _):
        off = pl.multiple_of(t * LANES, LANES)
        block = ell[:, pl.ds(off, LANES)]
        local = (block >= 0) & (block < nodes)
        wide_g = jnp.where(local, block & (words - 1), -1)
        wide_p = jnp.left_shift(jnp.ones_like(block), jnp.where(local, (block // words) * 4, 0))
        g = [jnp.broadcast_to(wide_g[s : s + 1, :], (8, LANES)) for s in range(slots)]
        p = [jnp.broadcast_to(wide_p[s : s + 1, :], (8, LANES)) for s in range(slots)]
        word = list(p)
        for i in range(slots):
            for j in range(i):
                same = g[i] == g[j]
                word[i] = word[i] + jnp.where(same, p[j], no_word)
                word[j] = word[j] + jnp.where(same, p[i], no_word)
        for h in range(0, words, 64):
            chunk = []
            for q in range(h, h + 64, 8):
                ids = word_ids + q
                acc = no_word
                for s in range(slots):
                    acc = jnp.where(g[s] == ids, word[s], acc)
                chunk.append(acc)
            chunk = jnp.concatenate(chunk, axis=0)
            for r in range(DIGITS):
                last = r == DIGITS - 1
                digit = lax.shift_right_logical(chunk, 4 * r) if last else chunk & (15 << (4 * r))
                adj[t, r * words + h : r * words + h + 64, :] = digit.astype(F32).astype(BF16)
        from_slot[t] = jnp.max(block, axis=0, keepdims=True) - nodes
        return 0

    def adj_block(b):
        return jnp.concatenate([adj[b // LANES], adj[b // LANES + 1]], axis=1)

    def scale_of(r):
        return 1.0 if r == DIGITS - 1 else 16.0**-r

    def split_field(v):
        for r in range(DIGITS):
            s = slice(r * words, (r + 1) * words)
            part = v[:, s] * scale_of(r)
            for i, piece in enumerate(pieces(part)):
                lhs[i * pairs : (i + 1) * pairs, s] = piece
            for i, piece in enumerate(pieces(part * cond[:, s])):
                lhs[(3 + i) * pairs : (4 + i) * pairs, s] = piece

    half = 0.5
    with jax.named_scope("adj_a"):
        loads[3].wait()
        ahead = jnp.where(place < group // 2, nodes // LANES, nodes // LANES // 4)
        lax.fori_loop(0, ahead, build, 0)
    with jax.named_scope("barwait"):
        pl.semaphore_wait(barrier, len(neighbours) + len(near) + len(far))
    ex0 = exchange(0, out0, in0)
    with jax.named_scope("adj_b"):
        lax.fori_loop(ahead, nodes // LANES, build, 0)

    def local_operator(v, y, first):
        rows = 7 * pairs if first else 6 * pairs
        for b in range(0, nodes, WIDE):
            s = slice(b, b + WIDE)
            prod = jnp.dot(lhs[0:rows, :], adj_block(b), preferred_element_type=F32)
            c = cond[:, s]
            if first:
                extra = prod[6 * pairs :]
                around = joined(extra, 0, 1)
                diag[:, s] = gnd[:, s] + half * (c * extra[3:4] + around)
            y[:, s] = diag[:, s] * v[:, s] - half * (c * joined(prod, 0, pairs) + joined(prod, 3 * pairs, pairs))

    def add_received(t, y, v):
        for k, s in enumerate(tiles(nodes)):
            slot = jnp.broadcast_to(from_slot[k], (8, LANES))
            lane, link = slot & (LANES - 1), lax.shift_right_arithmetic(slot, 7)
            found = [jnp.zeros((8, LANES), F32)] * (pairs // 8)
            for o, part in enumerate(tiles(bound)):
                here = link == o
                for i in range(pairs // 8):
                    found[i] = jnp.where(here, taken(t[i * 8 : i * 8 + 8, part], lane), found[i])
            v[:, s] = y[:, s] + jnp.concatenate(found, axis=0)

    def pass_on(y, u, out):
        for o, found in enumerate(picked(field_rows(y), pairs)):
            u[:, o * LANES : (o + 1) * LANES] = found
            out[o, :, :] = found

    def lane_sums(first, second):
        total = None
        for s in tiles(first.shape[1]):
            term = first[:, s] * second[:, s]
            total = term if total is None else total + term
        return total

    def row_of(sums):
        blocks = jnp.concatenate(sums + [jnp.zeros((LANES - pairs * len(sums), LANES), F32)], axis=0)
        return jnp.sum(jnp.transpose(blocks), axis=0, keepdims=True)

    def reduction(stage, peers):
        for d, peer in enumerate(peers, start=1):
            pltpu.make_async_remote_copy(
                src_ref=red.at[stage, 0],
                dst_ref=red.at[stage, d],
                send_sem=red_send.at[stage],
                recv_sem=red_recv.at[stage],
                device_id={"dom": peer},
                device_id_type=MESH,
            ).start()
        slots_used = red.at[stage, 1 : len(peers) + 1]
        return pltpu.make_async_remote_copy(
            src_ref=slots_used, dst_ref=slots_used, send_sem=red_send.at[stage], recv_sem=red_recv.at[stage],
            device_id={"dom": peers[0]}, device_id_type=MESH,
        )

    def summed(stage, count):
        terms = [red[stage, d] for d in range(count)]
        while len(terms) > 1:
            terms = [a + b for a, b in zip(terms[0::2], terms[1::2], strict=True)]
        return terms[0]

    def spread_row(row):
        return jnp.transpose(jnp.broadcast_to(row, (LANES, LANES)))

    lhs[6 * pairs :, :] = jnp.zeros((pairs, nodes), BF16)
    loads[2].wait()
    for r in range(DIGITS):
        s = slice(r * words, (r + 1) * words)
        for i, piece in enumerate(pieces(cond[:, s] * scale_of(r))):
            lhs[6 * pairs + i : 6 * pairs + i + 1, s] = piece
        lhs[6 * pairs + 3 : 6 * pairs + 4, s] = jnp.full((1, words), scale_of(r), BF16)
    split_field(cur)
    local_operator(cur, y0, True)
    pass_on(y0, u1, out1)
    ex1 = exchange(1, out1, in1)

    red[0, 0] = row_of([lane_sums(cur, cur), lane_sums(cur, y0)])
    near0 = reduction(0, near)

    def remote_terms(u, other, t):
        for o in range(links):
            s = slice(o * LANES, (o + 1) * LANES)
            weight = jnp.concatenate([wsend[:, s]] * (pairs // 8), axis=0)
            t[:, s] = weight * (u[:, s] - other(o, s))

    ex0.wait_recv()
    for o in range(links):
        s = slice(o * LANES, (o + 1) * LANES)
        live = jnp.broadcast_to(send[o : o + 1, :], (8, LANES)) >= 0
        wsend[:, s] = jnp.where(live, half * (wsend[:, s] + in0[o, pairs : pairs + 8, :]), 0.0)
    remote_terms(u0, lambda o, s: in0[o, 0:pairs, :], t0)
    add_received(t0, y0, v1)
    split_field(v1)
    local_operator(v1, y1, False)
    pass_on(y1, u2, out2)
    ex2 = exchange(2, out2, in2)

    near0.wait_recv()
    red[1, 0] = summed(0, group)
    far0 = reduction(1, far)

    ex1.wait_recv()
    u1[...] = u1[...] + t0[...]
    remote_terms(u1, lambda o, s: in1[o, :, :] - t0[:, s], t1)
    add_received(t1, y1, v2)
    split_field(v2)
    local_operator(v2, y2, False)

    ex2.wait_recv()
    u2[...] = u2[...] + t1[...]
    remote_terms(u2, lambda o, s: in2[o, :, :] - t1[:, s], t2)
    far0.wait_recv()
    first_sums = spread_row(summed(1, others))
    step = first_sums[0:pairs] / first_sums[pairs : 2 * pairs]

    zero = jnp.zeros((pairs, LANES), F32)
    g0, g1, h0, h1, h2, h3 = zero, zero, zero, zero, zero, zero
    for s in tiles(nodes):
        w = cur[:, s] - step * v1[:, s]
        z = v1[:, s] - step * v2[:, s]
        g0 = g0 + cur[:, s] * cur[:, s]
        g1 = g1 + cur[:, s] * w
        h0 = h0 + w * w
        h1 = h1 + w * z
        h2 = h2 + z * z
        h3 = h3 + z * (y1[:, s] - step * y2[:, s])
    for s in tiles(bound):
        h3 = h3 + (u1[:, s] - step * u2[:, s]) * (t1[:, s] - step * t2[:, s])
    red[2, 0] = row_of([g0, g1, h0, h1, h2, h3])
    near1 = reduction(2, near)

    add_received(t2, y2, v3)

    near1.wait_recv()
    red[3, 0] = summed(2, group)
    far1 = reduction(3, far)
    far1.wait_recv()
    sums = spread_row(summed(3, others))
    m0, g1, h0, h1, h2, h3 = (sums[i * pairs : (i + 1) * pairs] for i in range(6))

    tilt = g1 / (m0 - g1)
    lead = 1.0 + tilt
    a0 = step * lead
    rz = (g1 - h0) / step
    az = (rz - h1) / step
    aa = (m0 - 2.0 * g1 + h0) / (step * step)
    aaz = (az - h2) / step
    aaa = (aa - az) / step
    k0 = lead * (lead * h0 - tilt * g1)
    k1 = lead * (lead * h1 - tilt * rz) + tilt * k0 / a0
    k2 = lead * (lead * h2 - 2.0 * tilt * az) + tilt * tilt * aa
    k3 = lead * (lead * h3 - 2.0 * tilt * aaz) + tilt * tilt * aaa

    b1 = k0 / m0
    a1 = k0 / (k1 - b1 * k0 / a0)
    v1q1 = -(k0 / a0 + k1) / a0
    r2q1 = k1 - a1 * (k2 + b1 * v1q1)
    rr2 = -a1 * r2q1
    b2 = rr2 / k0
    v1q2 = (v1q1 - k2) / a0
    r2q2 = k2 - a1 * (k3 + b1 * v1q2)
    r2ar2 = r2q1 - a1 * (r2q2 - b1 * r2q1 / a0)
    a2 = rr2 / (r2ar2 - b2 * rr2 / a1)

    for s in tiles(nodes):
        w0, w1, w2, w3 = cur[:, s], v1[:, s], v2[:, s], v3[:, s]
        r1 = w0 - a0 * w1
        q1 = w1 - a0 * w2
        q2 = w2 - a0 * w3
        p1 = r1 + b1 * w0
        ap1 = q1 + b1 * w1
        r2 = r1 - a1 * ap1
        ar2 = q1 - a1 * (q2 + b1 * w2)
        p2 = r2 + b2 * p1
        ap2 = ar2 + b2 * ap1
        volt[:, s] = a0 * w0 + a1 * p1 + a2 * p2
        resid[:, s] = r2 - a2 * ap2

    for copies in (ex0, ex1, ex2, near0, far0, near1, far1):
        copies.wait_send()


def write_out(volt, resid, volt_out, resid_out, sems):
    copies = [pltpu.make_async_copy(volt, volt_out, sems.at[0]), pltpu.make_async_copy(resid, resid_out, sems.at[1])]
    for copy in copies:
        copy.start()
    for copy in copies:
        copy.wait()


def solve(parts, group, currents, conductance, ground, ell_cols, send_rows):
    pairs, nodes = currents.shape
    links = send_rows.shape[0]
    bound = links * LANES
    others = parts // group
    most = max(group, others)
    field = pltpu.VMEM((pairs, nodes), F32)
    edge = pltpu.VMEM((pairs, bound), F32)
    vmem = pl.BlockSpec(memory_space=pltpu.VMEM)
    volt, resid = pl.pallas_call(
        functools.partial(kernel, parts, group),
        out_shape=(jax.ShapeDtypeStruct((pairs, nodes), F32),) * 2,
        in_specs=[pl.BlockSpec(memory_space=pltpu.HBM)] * 5,
        out_specs=(vmem, vmem),
        scratch_shapes=[
            field,
            pltpu.VMEM((1, nodes), F32),
            pltpu.VMEM((1, nodes), F32),
            pltpu.VMEM(ell_cols.shape, I32),
            pltpu.VMEM(send_rows.shape, I32),
            pltpu.SemaphoreType.DMA((5,)),
            pltpu.VMEM((nodes // LANES, nodes, LANES), BF16),
            pltpu.VMEM((nodes // LANES, 1, LANES), I32),
            field, field, field, field, field, field,
            pltpu.VMEM((1, nodes), F32),
            pltpu.VMEM((7 * pairs, nodes), BF16),
            pltpu.VMEM((8, bound), F32),
            edge, edge, edge, edge, edge, edge,
            pltpu.VMEM((links, pairs + 8, LANES), F32),
            pltpu.VMEM((links, pairs, LANES), F32),
            pltpu.VMEM((links, pairs, LANES), F32),
            pltpu.VMEM((links, pairs + 8, LANES), F32),
            pltpu.VMEM((links, pairs, LANES), F32),
            pltpu.VMEM((links, pairs, LANES), F32),
            pltpu.VMEM((4, most, 1, LANES), F32),
            pltpu.SemaphoreType.DMA((3,)),
            pltpu.SemaphoreType.DMA((3,)),
            pltpu.SemaphoreType.DMA((4,)),
            pltpu.SemaphoreType.DMA((4,)),
        ],
        compiler_params=pltpu.CompilerParams(
            collective_id=0, has_side_effects=True, vmem_limit_bytes=48 * 1024 * 1024
        ),
    )(*(pltpu.with_memory_space_constraint(x, pltpu.HBM) for x in (currents, conductance.reshape(1, nodes), ground.reshape(1, nodes), ell_cols, send_rows)))
    return pl.pallas_call(
        write_out,
        out_shape=(jax.ShapeDtypeStruct((pairs, nodes), F32),) * 2,
        in_specs=[vmem] * 2,
        out_specs=(pl.BlockSpec(memory_space=pltpu.HBM),) * 2,
        scratch_shapes=[pltpu.SemaphoreType.DMA((2,))],
        compiler_params=pltpu.CompilerParams(vmem_limit_bytes=1 << 20),
    )(volt, resid)


def solution(mesh):
    parts = mesh.shape["dom"]
    group = 16 if parts >= 256 else 4
    placed = (P(None, "dom"), P("dom"), P("dom"), P(None, "dom"), P("dom", None))
    return jax.shard_map(
        functools.partial(solve, parts, group),
        mesh=mesh,
        in_specs=placed,
        out_specs=(P(None, "dom"), P(None, "dom")),
        check_vma=False,
    )
```

```python
import functools

import jax
import jax.numpy as jnp
from jax import lax
from jax.experimental import pallas as pl
from jax.experimental.pallas import tpu as pltpu
from jax.sharding import PartitionSpec as P

MESH = pl.DeviceIdType.MESH
F32, BF16, I32 = jnp.float32, jnp.bfloat16, jnp.int32
LANES = 128
WIDE = 256
DIGITS = 8


def pieces(x):
    high = x.astype(BF16)
    rest = x - high.astype(F32)
    mid = rest.astype(BF16)
    low = (rest - mid.astype(F32)).astype(BF16)
    return [high, mid, low]


def joined(y, first, rows):
    return (y[first + 2 * rows : first + 3 * rows] + y[first + rows : first + 2 * rows]) + y[first : first + rows]


def two_sum(a, b):
    s = a + b
    part = s - a
    return s, (a - (s - part)) + (b - part)


def two_product(a, b):
    p = a * b
    wide_a, wide_b = a * 4097.0, b * 4097.0
    a1 = wide_a - (wide_a - a)
    b1 = wide_b - (wide_b - b)
    a2, b2 = a - a1, b - b1
    return p, ((a1 * b1 - p) + a1 * b2 + a2 * b1) + a2 * b2


def pair_add(a, b):
    s, e = two_sum(a[0], b[0])
    e = e + (a[1] + b[1])
    high = s + e
    return high, e - (high - s)


def tree(terms, add):
    while len(terms) > 1:
        terms = [add(a, b) for a, b in zip(terms[0::2], terms[1::2], strict=True)]
    return terms[0]


def tiles(width):
    return [slice(i, i + LANES) for i in range(0, width, LANES)]


def kernel(
    parts, group, cur_in, cond_in, gnd_in, ell_in, send_in, volt, resid,
    cur, cond, gnd, ell, send, in_sem, adj, from_slot, v1, v2, v3, y0, y1, y2, diag, lhs, wsend, u0, u1, u2, t0, t1, t2,
    out0, out1, out2, in0, in1, in2, red, ex_send, ex_recv, red_send, red_recv,
):
    pairs, nodes = cur.shape
    slots = ell.shape[0]
    links = send.shape[0]
    bound = links * LANES
    reach = links // 2
    offsets = list(range(-reach, 0)) + list(range(1, reach + 1))
    me = lax.axis_index("dom")
    others = parts // group
    mine, place = me // group, me % group

    assert reach == 3
    neighbours, landing = [], []
    for o, e in enumerate(offsets):
        d = abs(e)
        edge = me if e < 0 else parts - 1 - me
        spare = jnp.where(edge == 0, 1 if d < 3 else 2, 0)
        spare_d = jnp.where(edge == 0, min(d + 1, 3), jnp.where(edge == 1, d - 1, 3))
        inside = edge >= d
        spare_peer = spare if e < 0 else parts - 1 - spare
        spare_slot = reach - spare_d if e < 0 else reach - 1 + spare_d
        neighbours.append(jnp.where(inside, me + e, spare_peer))
        landing.append(jnp.where(inside, links - 1 - o, spare_slot))
    near = [mine * group + lax.rem(place + d, group) for d in range(1, group)]
    far = [lax.rem(mine + d, others) * group + place for d in range(1, others)]

    barrier = pltpu.get_barrier_semaphore()
    for peer in far + near[group // 2 - 1 :] + near[: group // 2 - 1] + neighbours:
        pl.semaphore_signal(barrier, inc=1, device_id={"dom": peer}, device_id_type=MESH)
    loads = [
        pltpu.make_async_copy(source, target, in_sem.at[i])
        for i, (source, target) in enumerate(
            ((cur_in, cur), (cond_in, cond), (gnd_in, gnd), (ell_in, ell), (send_in, send))
        )
    ]
    loads[4].start()
    loads[0].start()
    for i in range(1, 4):
        loads[i].start()

    word_ids = lax.broadcasted_iota(I32, (8, LANES), 0)
    no_word = jnp.zeros((8, LANES), I32)
    words = nodes // DIGITS

    def taken(x, lane):
        return jnp.take_along_axis(x, lane, axis=1, mode="promise_in_bounds")

    def picked(source, rows):
        found = []
        for o in range(links):
            node = jnp.broadcast_to(send[o : o + 1, :], (8, LANES))
            lane, tile = node & (LANES - 1), lax.shift_right_arithmetic(node, 7)
            parts_found = [jnp.zeros((8, LANES), F32)] * (rows // 8)
            for k, s in enumerate(tiles(nodes)):
                here = tile == k
                for i in range(rows // 8):
                    parts_found[i] = jnp.where(here, taken(source(i, s), lane), parts_found[i])
            found.append(jnp.concatenate(parts_found, axis=0))
        return found

    def field_rows(field):
        return lambda i, s: field[i * 8 : i * 8 + 8, s]

    with jax.named_scope("pick_cur"):
        loads[4].wait()
        loads[0].wait()
        loads[1].wait()
        for o, (u, c) in enumerate(
            zip(
                picked(field_rows(cur), pairs),
                picked(lambda i, s: jnp.broadcast_to(cond[:, s], (8, LANES)), 8),
                strict=True,
            )
        ):
            s = slice(o * LANES, (o + 1) * LANES)
            u0[:, s] = u
            wsend[:, s] = c
            out0[o, 0:pairs, :] = u
            out0[o, pairs : pairs + 8, :] = c

    def exchange(step, out, into):
        for o in range(links):
            pltpu.make_async_remote_copy(
                src_ref=out.at[o],
                dst_ref=into.at[landing[o]],
                send_sem=ex_send.at[step],
                recv_sem=ex_recv.at[step],
                device_id={"dom": neighbours[o]},
                device_id_type=MESH,
            ).start()
        return pltpu.make_async_remote_copy(
            src_ref=out, dst_ref=into, send_sem=ex_send.at[step], recv_sem=ex_recv.at[step],
            device_id={"dom": neighbours[0]}, device_id_type=MESH,
        )

    def build(t, _):
        off = pl.multiple_of(t * LANES, LANES)
        block = ell[:, pl.ds(off, LANES)]
        local = (block >= 0) & (block < nodes)
        wide_g = jnp.where(local, block & (words - 1), -1)
        wide_p = jnp.left_shift(jnp.ones_like(block), jnp.where(local, (block // words) * 4, 0))
        g = [jnp.broadcast_to(wide_g[s : s + 1, :], (8, LANES)) for s in range(slots)]
        p = [jnp.broadcast_to(wide_p[s : s + 1, :], (8, LANES)) for s in range(slots)]
        word = list(p)
        for i in range(slots):
            for j in range(i):
                same = g[i] == g[j]
                word[i] = word[i] + jnp.where(same, p[j], no_word)
                word[j] = word[j] + jnp.where(same, p[i], no_word)
        for h in range(0, words, 64):
            chunk = []
            for q in range(h, h + 64, 8):
                ids = word_ids + q
                acc = no_word
                for s in range(slots):
                    acc = jnp.where(g[s] == ids, word[s], acc)
                chunk.append(acc)
            chunk = jnp.concatenate(chunk, axis=0)
            for r in range(DIGITS):
                last = r == DIGITS - 1
                digit = lax.shift_right_logical(chunk, 4 * r) if last else chunk & (15 << (4 * r))
                adj[t, r * words + h : r * words + h + 64, :] = digit.astype(F32).astype(BF16)
        from_slot[t] = jnp.max(block, axis=0, keepdims=True) - nodes
        return 0

    def adj_block(b):
        return jnp.concatenate([adj[b // LANES], adj[b // LANES + 1]], axis=1)

    def scale_of(r):
        return 1.0 if r == DIGITS - 1 else 16.0**-r

    def split_field(v):
        for r in range(DIGITS):
            s = slice(r * words, (r + 1) * words)
            part = v[:, s] * scale_of(r)
            for i, piece in enumerate(pieces(part)):
                lhs[i * pairs : (i + 1) * pairs, s] = piece
            for i, piece in enumerate(pieces(part * cond[:, s])):
                lhs[(3 + i) * pairs : (4 + i) * pairs, s] = piece

    half = 0.5
    with jax.named_scope("adj_a"):
        loads[3].wait()
        ahead = jnp.where(place < group // 2, nodes // LANES, nodes // LANES // 4)
        lax.fori_loop(0, ahead, build, 0)
    with jax.named_scope("barwait"):
        pl.semaphore_wait(barrier, len(neighbours) + len(near) + len(far))
    ex0 = exchange(0, out0, in0)
    with jax.named_scope("adj_b"):
        lax.fori_loop(ahead, nodes // LANES, build, 0)

    def local_operator(v, y, first):
        rows = 7 * pairs if first else 6 * pairs
        for b in range(0, nodes, WIDE):
            s = slice(b, b + WIDE)
            prod = jnp.dot(lhs[0:rows, :], adj_block(b), preferred_element_type=F32)
            c = cond[:, s]
            if first:
                extra = prod[6 * pairs :]
                around = joined(extra, 0, 1)
                diag[:, s] = gnd[:, s] + half * (c * extra[3:4] + around)
            y[:, s] = diag[:, s] * v[:, s] - half * (c * joined(prod, 0, pairs) + joined(prod, 3 * pairs, pairs))

    def add_received(t, y, v):
        for k, s in enumerate(tiles(nodes)):
            slot = jnp.broadcast_to(from_slot[k], (8, LANES))
            lane, link = slot & (LANES - 1), lax.shift_right_arithmetic(slot, 7)
            found = [jnp.zeros((8, LANES), F32)] * (pairs // 8)
            for o, part in enumerate(tiles(bound)):
                here = link == o
                for i in range(pairs // 8):
                    found[i] = jnp.where(here, taken(t[i * 8 : i * 8 + 8, part], lane), found[i])
            v[:, s] = y[:, s] + jnp.concatenate(found, axis=0)

    def pass_on(y, u, out):
        for o, found in enumerate(picked(field_rows(y), pairs)):
            u[:, o * LANES : (o + 1) * LANES] = found
            out[o, :, :] = found

    def lane_sums(first, second):
        total = None
        for s in tiles(first.shape[1]):
            term = first[:, s] * second[:, s]
            total = term if total is None else total + term
        return total

    def send_row(sums):
        blocks = jnp.concatenate(sums + [jnp.zeros((LANES - pairs * len(sums), LANES), F32)], axis=0)
        turned = jnp.transpose(blocks)
        total = tree([two_sum(turned[i : i + 8], turned[i + 8 : i + 16]) for i in range(0, LANES, 16)], pair_add)
        for shift in (4, 2, 1):
            total = pair_add(total, tuple(pltpu.roll(x, shift, axis=0) for x in total))
        put_row(0, total)

    def put_row(stage, total):
        red[stage, 0, 0:1, :] = total[0][0:1]
        red[stage, 0, 1:2, :] = total[1][0:1]

    def reduction(stage, peers):
        for d, peer in enumerate(peers, start=1):
            pltpu.make_async_remote_copy(
                src_ref=red.at[stage, 0],
                dst_ref=red.at[stage, d],
                send_sem=red_send.at[stage],
                recv_sem=red_recv.at[stage],
                device_id={"dom": peer},
                device_id_type=MESH,
            ).start()
        slots_used = red.at[stage, 1 : len(peers) + 1]
        return pltpu.make_async_remote_copy(
            src_ref=slots_used, dst_ref=slots_used, send_sem=red_send.at[stage], recv_sem=red_recv.at[stage],
            device_id={"dom": peers[0]}, device_id_type=MESH,
        )

    def summed(stage, count):
        return tree([(red[stage, d, 0:1, :], red[stage, d, 1:2, :]) for d in range(count)], pair_add)

    def spread_row(row):
        return jnp.transpose(jnp.broadcast_to(row, (LANES, LANES)))

    lhs[6 * pairs :, :] = jnp.zeros((pairs, nodes), BF16)
    loads[2].wait()
    for r in range(DIGITS):
        s = slice(r * words, (r + 1) * words)
        for i, piece in enumerate(pieces(cond[:, s] * scale_of(r))):
            lhs[6 * pairs + i : 6 * pairs + i + 1, s] = piece
        lhs[6 * pairs + 3 : 6 * pairs + 4, s] = jnp.full((1, words), scale_of(r), BF16)
    split_field(cur)
    local_operator(cur, y0, True)
    pass_on(y0, u1, out1)
    ex1 = exchange(1, out1, in1)

    def remote_terms(u, other, t):
        for o in range(links):
            s = slice(o * LANES, (o + 1) * LANES)
            weight = jnp.concatenate([wsend[:, s]] * (pairs // 8), axis=0)
            t[:, s] = weight * (u[:, s] - other(o, s))

    ex0.wait_recv()
    for o in range(links):
        s = slice(o * LANES, (o + 1) * LANES)
        live = jnp.broadcast_to(send[o : o + 1, :], (8, LANES)) >= 0
        wsend[:, s] = jnp.where(live, half * (wsend[:, s] + in0[o, pairs : pairs + 8, :]), 0.0)
    remote_terms(u0, lambda o, s: in0[o, 0:pairs, :], t0)
    add_received(t0, y0, v1)
    split_field(v1)
    local_operator(v1, y1, False)
    pass_on(y1, u2, out2)
    ex2 = exchange(2, out2, in2)
    moments = [lane_sums(cur, cur), lane_sums(cur, v1), lane_sums(v1, v1)]

    ex1.wait_recv()
    u1[...] = u1[...] + t0[...]
    remote_terms(u1, lambda o, s: in1[o, :, :] - t0[:, s], t1)
    add_received(t1, y1, v2)
    split_field(v2)
    moments += [lane_sums(v1, v2), lane_sums(v2, v2)]
    local_operator(v2, y2, False)

    ex2.wait_recv()
    u2[...] = u2[...] + t1[...]
    remote_terms(u2, lambda o, s: in2[o, :, :] - t1[:, s], t2)
    moments.append(lane_sums(v2, y2) + lane_sums(u2, t2))
    send_row(moments)
    near_sums = reduction(0, near)

    add_received(t2, y2, v3)

    near_sums.wait_recv()
    put_row(1, summed(0, group))
    far_sums = reduction(1, far)
    far_sums.wait_recv()
    high, low = (spread_row(x) for x in summed(1, others))
    m = [(high[i * pairs : (i + 1) * pairs], low[i * pairs : (i + 1) * pairs]) for i in range(6)]

    m0 = m[0][0]
    a0 = m0 / m[1][0]
    square, square_rest = two_product(a0, a0)
    double = 2.0 * a0

    def shifted(i):
        p, p_rest = two_product(m[i + 1][0], double)
        q, q_rest = two_product(m[i + 2][0], square)
        p_rest = p_rest + m[i + 1][1] * double
        q_rest = q_rest + (m[i + 2][1] * square + m[i + 2][0] * square_rest)
        s, s_rest = two_sum(m[i][0], -p)
        s, t_rest = two_sum(s, q)
        return s + ((s_rest + t_rest) + (m[i][1] - p_rest + q_rest))

    k0, k1, k2, k3 = (shifted(i) for i in range(4))

    b1 = k0 / m0
    a1 = k0 / (k1 - b1 * k0 / a0)
    v1q1 = -(k0 / a0 + k1) / a0
    r2q1 = k1 - a1 * (k2 + b1 * v1q1)
    rr2 = -a1 * r2q1
    b2 = rr2 / k0
    v1q2 = (v1q1 - k2) / a0
    r2q2 = k2 - a1 * (k3 + b1 * v1q2)
    r2ar2 = r2q1 - a1 * (r2q2 - b1 * r2q1 / a0)
    a2 = rr2 / (r2ar2 - b2 * rr2 / a1)

    for s in tiles(nodes):
        w0, w1, w2, w3 = cur[:, s], v1[:, s], v2[:, s], v3[:, s]
        r1 = w0 - a0 * w1
        q1 = w1 - a0 * w2
        q2 = w2 - a0 * w3
        p1 = r1 + b1 * w0
        ap1 = q1 + b1 * w1
        r2 = r1 - a1 * ap1
        ar2 = q1 - a1 * (q2 + b1 * w2)
        p2 = r2 + b2 * p1
        ap2 = ar2 + b2 * ap1
        volt[:, s] = a0 * w0 + a1 * p1 + a2 * p2
        resid[:, s] = r2 - a2 * ap2

    for copies in (ex0, ex1, ex2, near_sums, far_sums):
        copies.wait_send()


def write_out(volt, resid, volt_out, resid_out, sems):
    copies = [pltpu.make_async_copy(volt, volt_out, sems.at[0]), pltpu.make_async_copy(resid, resid_out, sems.at[1])]
    for copy in copies:
        copy.start()
    for copy in copies:
        copy.wait()


def solve(parts, group, currents, conductance, ground, ell_cols, send_rows):
    pairs, nodes = currents.shape
    links = send_rows.shape[0]
    bound = links * LANES
    others = parts // group
    most = max(group, others)
    field = pltpu.VMEM((pairs, nodes), F32)
    edge = pltpu.VMEM((pairs, bound), F32)
    vmem = pl.BlockSpec(memory_space=pltpu.VMEM)
    volt, resid = pl.pallas_call(
        functools.partial(kernel, parts, group),
        out_shape=(jax.ShapeDtypeStruct((pairs, nodes), F32),) * 2,
        in_specs=[pl.BlockSpec(memory_space=pltpu.HBM)] * 5,
        out_specs=(vmem, vmem),
        scratch_shapes=[
            field,
            pltpu.VMEM((1, nodes), F32),
            pltpu.VMEM((1, nodes), F32),
            pltpu.VMEM(ell_cols.shape, I32),
            pltpu.VMEM(send_rows.shape, I32),
            pltpu.SemaphoreType.DMA((5,)),
            pltpu.VMEM((nodes // LANES, nodes, LANES), BF16),
            pltpu.VMEM((nodes // LANES, 1, LANES), I32),
            field, field, field, field, field, field,
            pltpu.VMEM((1, nodes), F32),
            pltpu.VMEM((7 * pairs, nodes), BF16),
            pltpu.VMEM((8, bound), F32),
            edge, edge, edge, edge, edge, edge,
            pltpu.VMEM((links, pairs + 8, LANES), F32),
            pltpu.VMEM((links, pairs, LANES), F32),
            pltpu.VMEM((links, pairs, LANES), F32),
            pltpu.VMEM((links, pairs + 8, LANES), F32),
            pltpu.VMEM((links, pairs, LANES), F32),
            pltpu.VMEM((links, pairs, LANES), F32),
            pltpu.VMEM((2, most, 2, LANES), F32),
            pltpu.SemaphoreType.DMA((3,)),
            pltpu.SemaphoreType.DMA((3,)),
            pltpu.SemaphoreType.DMA((2,)),
            pltpu.SemaphoreType.DMA((2,)),
        ],
        compiler_params=pltpu.CompilerParams(
            collective_id=0, has_side_effects=True, vmem_limit_bytes=48 * 1024 * 1024
        ),
    )(*(pltpu.with_memory_space_constraint(x, pltpu.HBM) for x in (currents, conductance.reshape(1, nodes), ground.reshape(1, nodes), ell_cols, send_rows)))
    return pl.pallas_call(
        write_out,
        out_shape=(jax.ShapeDtypeStruct((pairs, nodes), F32),) * 2,
        in_specs=[vmem] * 2,
        out_specs=(pl.BlockSpec(memory_space=pltpu.HBM),) * 2,
        scratch_shapes=[pltpu.SemaphoreType.DMA((2,))],
        compiler_params=pltpu.CompilerParams(vmem_limit_bytes=1 << 20),
    )(volt, resid)


def solution(mesh):
    parts = mesh.shape["dom"]
    group = 16 if parts >= 256 else 4
    placed = (P(None, "dom"), P("dom"), P("dom"), P(None, "dom"), P("dom", None))
    return jax.shard_map(
        functools.partial(solve, parts, group),
        mesh=mesh,
        in_specs=placed,
        out_specs=(P(None, "dom"), P(None, "dom")),
        check_vma=False,
    )
```

```python
import functools

import jax
import jax.numpy as jnp
from jax import lax
from jax.experimental import pallas as pl
from jax.experimental.pallas import tpu as pltpu
from jax.sharding import PartitionSpec as P

MESH = pl.DeviceIdType.MESH
F32, BF16, I32 = jnp.float32, jnp.bfloat16, jnp.int32
LANES = 128
WIDE = 256
DIGITS = 8


def pieces(x):
    high = x.astype(BF16)
    rest = x - high.astype(F32)
    mid = rest.astype(BF16)
    low = (rest - mid.astype(F32)).astype(BF16)
    return [high, mid, low]


def joined(y, first, rows):
    return (y[first + 2 * rows : first + 3 * rows] + y[first + rows : first + 2 * rows]) + y[first : first + rows]


def two_sum(a, b):
    s = a + b
    part = s - a
    return s, (a - (s - part)) + (b - part)


def two_product(a, b):
    p = a * b
    wide_a, wide_b = a * 4097.0, b * 4097.0
    a1 = wide_a - (wide_a - a)
    b1 = wide_b - (wide_b - b)
    a2, b2 = a - a1, b - b1
    return p, ((a1 * b1 - p) + a1 * b2 + a2 * b1) + a2 * b2


def pair_add(a, b):
    s, e = two_sum(a[0], b[0])
    e = e + (a[1] + b[1])
    high = s + e
    return high, e - (high - s)


def tree(terms, add):
    while len(terms) > 1:
        terms = [add(a, b) for a, b in zip(terms[0::2], terms[1::2], strict=True)]
    return terms[0]


def tiles(width):
    return [slice(i, i + LANES) for i in range(0, width, LANES)]


def kernel(
    parts, group, cur_in, cond_in, gnd_in, ell_in, send_in, volt, resid,
    cur, cond, gnd, ell, send, in_sem, adj, from_slot, v1, v2, v3, y0, y1, y2, diag, lhs, wsend, u0, u1, u2, t0, t1, t2,
    out0, out1, out2, in0, in1, in2, red, ex_send, ex_recv, red_send, red_recv,
):
    pairs, nodes = cur.shape
    slots = ell.shape[0]
    links = send.shape[0]
    bound = links * LANES
    reach = links // 2
    offsets = list(range(-reach, 0)) + list(range(1, reach + 1))
    me = lax.axis_index("dom")
    others = parts // group
    mine, place = me // group, me % group

    assert reach == 3
    neighbours, landing, side_of = [], [], []
    for o, e in enumerate(offsets):
        d = abs(e)
        edge = me if e < 0 else parts - 1 - me
        spare = jnp.where(edge == 0, 1 if d < 3 else 2, 0)
        spare_d = jnp.where(edge == 0, min(d + 1, 3), jnp.where(edge == 1, d - 1, 3))
        inside = edge >= d
        spare_peer = spare if e < 0 else parts - 1 - spare
        spare_slot = reach - spare_d if e < 0 else reach - 1 + spare_d
        neighbours.append(jnp.where(inside, me + e, spare_peer))
        landing.append(jnp.where(inside, links - 1 - o, spare_slot))
        side_of.append(jnp.where(inside, 1 if e < 0 else 0, 0 if e < 0 else 1))
    def steps(d, count):
        return min(d, count - d)

    near = [
        (d, mine * group + lax.rem(place + d, group))
        for d in sorted(range(1, group), key=lambda d: -steps(d, group))
    ]
    side = 4 if others == 16 else 2
    row, column = mine // side, mine % side
    far = [
        (d, (lax.rem(row + d // side, side) * side + lax.rem(column + d % side, side)) * group + place)
        for d in sorted(range(1, others), key=lambda d: -steps(d // side, side) - steps(d % side, side))
    ]

    loads = [
        pltpu.make_async_copy(source, target, in_sem.at[i])
        for i, (source, target) in enumerate(
            ((cur_in, cur), (cond_in, cond), (gnd_in, gnd), (ell_in, ell), (send_in, send))
        )
    ]
    loads[4].start()
    loads[0].start()
    for i in range(1, 4):
        loads[i].start()

    barrier = pltpu.get_barrier_semaphore()
    for peer in neighbours + [peer for _, peer in near + far]:
        pl.semaphore_signal(barrier, inc=1, device_id={"dom": peer}, device_id_type=MESH)
    word_ids = lax.broadcasted_iota(I32, (8, LANES), 0)
    no_word = jnp.zeros((8, LANES), I32)
    words = nodes // DIGITS

    def taken(x, lane):
        return jnp.take_along_axis(x, lane, axis=1, mode="promise_in_bounds")

    def places(o):
        node = jnp.broadcast_to(send[o : o + 1, :], (8, LANES))
        return node & (LANES - 1), lax.shift_right_arithmetic(node, 7)

    def picked(source, rows):
        found = []
        for o in range(links):
            lane, tile = places(o)
            parts_found = [jnp.zeros((8, LANES), F32)] * (rows // 8)
            for k, s in enumerate(tiles(nodes)):
                here = tile == k
                for i in range(rows // 8):
                    parts_found[i] = jnp.where(here, taken(source(i, s), lane), parts_found[i])
            found.append(jnp.concatenate(parts_found, axis=0))
        return found

    def field_rows(field):
        return lambda i, s: field[i * 8 : i * 8 + 8, s]

    with jax.named_scope("pick_cur"):
        loads[4].wait()
        loads[0].wait()
        loads[1].wait()
        for o, (u, c) in enumerate(
            zip(
                picked(field_rows(cur), pairs),
                picked(lambda i, s: jnp.broadcast_to(cond[:, s], (8, LANES)), 8),
                strict=True,
            )
        ):
            s = slice(o * LANES, (o + 1) * LANES)
            u0[:, s] = u
            wsend[:, s] = c
            out0[o, 0:pairs, :] = u
            out0[o, pairs : pairs + 1, :] = c[0:1]

    def exchange(step, out, into):
        for o in sorted(range(links), key=lambda o: -abs(offsets[o])):
            pltpu.make_async_remote_copy(
                src_ref=out.at[o],
                dst_ref=into.at[landing[o]],
                send_sem=ex_send.at[step],
                recv_sem=ex_recv.at[step, side_of[o]],
                device_id={"dom": neighbours[o]},
                device_id_type=MESH,
            ).start()
        return [
            pltpu.make_async_remote_copy(
                src_ref=out.at[half], dst_ref=into.at[half], send_sem=ex_send.at[step], recv_sem=ex_recv.at[step, i],
                device_id={"dom": neighbours[0]}, device_id_type=MESH,
            )
            for i, half in enumerate((slice(0, reach), slice(reach, links)))
        ]

    def build(t, _):
        off = pl.multiple_of(t * LANES, LANES)
        block = ell[:, pl.ds(off, LANES)]
        local = (block >= 0) & (block < nodes)
        wide_g = jnp.where(local, block & (words - 1), -1)
        wide_p = jnp.left_shift(jnp.ones_like(block), jnp.where(local, (block // words) * 4, 0))
        g = [jnp.broadcast_to(wide_g[s : s + 1, :], (8, LANES)) for s in range(slots)]
        p = [jnp.broadcast_to(wide_p[s : s + 1, :], (8, LANES)) for s in range(slots)]
        word = list(p)
        for i in range(slots):
            for j in range(i):
                same = g[i] == g[j]
                word[i] = word[i] + jnp.where(same, p[j], no_word)
                word[j] = word[j] + jnp.where(same, p[i], no_word)
        for h in range(0, words, 64):
            chunk = []
            for q in range(h, h + 64, 8):
                ids = word_ids + q
                acc = no_word
                for s in range(slots):
                    acc = jnp.where(g[s] == ids, word[s], acc)
                chunk.append(acc)
            chunk = jnp.concatenate(chunk, axis=0)
            for r in range(DIGITS):
                last = r == DIGITS - 1
                digit = lax.shift_right_logical(chunk, 4 * r) if last else chunk & (15 << (4 * r))
                adj[t, r * words + h : r * words + h + 64, :] = digit.astype(F32).astype(BF16)
        from_slot[t] = jnp.max(block, axis=0, keepdims=True) - nodes
        return 0

    def adj_block(b):
        return jnp.concatenate([adj[b // LANES], adj[b // LANES + 1]], axis=1)

    def scale_of(r):
        return 1.0 if r == DIGITS - 1 else 16.0**-r

    def split_part(value, s):
        part = value * scale_of(s.start // words)
        for i, piece in enumerate(pieces(part)):
            lhs[i * pairs : (i + 1) * pairs, s] = piece
        for i, piece in enumerate(pieces(part * cond[:, s])):
            lhs[(3 + i) * pairs : (4 + i) * pairs, s] = piece

    half = 0.5
    with jax.named_scope("adj_a"):
        loads[3].wait()
        ahead = jnp.where(place < group // 2, nodes // LANES, nodes // LANES * 7 // 16)
        lax.fori_loop(0, ahead, build, 0)
    with jax.named_scope("barwait"):
        pl.semaphore_wait(barrier, len(neighbours) + len(near) + len(far))
    ex0 = exchange(0, out0, in0)
    with jax.named_scope("adj_b"):
        lax.fori_loop(ahead, nodes // LANES, build, 0)

    def local_operator(v, y, first, u=None, out=None):
        if u is not None:
            listed = [places(o) for o in range(links)]
            found = [[jnp.zeros((8, LANES), F32)] * (pairs // 8) for _ in range(links)]
        rows = 7 * pairs if first else 6 * pairs
        for b in range(0, nodes, WIDE):
            s = slice(b, b + WIDE)
            prod = jnp.dot(lhs[0:rows, :], adj_block(b), preferred_element_type=F32)
            c = cond[:, s]
            if first:
                extra = prod[6 * pairs :]
                around = joined(extra, 0, 1)
                diag[:, s] = gnd[:, s] + half * (c * extra[3:4] + around)
            result = diag[:, s] * v[:, s] - half * (c * joined(prod, 0, pairs) + joined(prod, 3 * pairs, pairs))
            y[:, s] = result
            if u is not None:
                for k in (b // LANES, b // LANES + 1):
                    inner = k * LANES - b
                    for o, (lane, tile) in enumerate(listed):
                        here = tile == k
                        for i in range(pairs // 8):
                            piece = result[i * 8 : i * 8 + 8, inner : inner + LANES]
                            found[o][i] = jnp.where(here, taken(piece, lane), found[o][i])
        if u is not None:
            for o in range(links):
                both = jnp.concatenate(found[o], axis=0)
                u[:, o * LANES : (o + 1) * LANES] = both
                out[o, :, :] = both

    def add_received(t, y, v, onward):
        for k, s in enumerate(tiles(nodes)):
            slot = jnp.broadcast_to(from_slot[k], (8, LANES))
            lane, link = slot & (LANES - 1), lax.shift_right_arithmetic(slot, 7)
            found = [jnp.zeros((8, LANES), F32)] * (pairs // 8)
            for o, part in enumerate(tiles(bound)):
                here = link == o
                for i in range(pairs // 8):
                    found[i] = jnp.where(here, taken(t[i * 8 : i * 8 + 8, part], lane), found[i])
            value = y[:, s] + jnp.concatenate(found, axis=0)
            v[:, s] = value
            if onward:
                split_part(value, s)

    def lane_sums(first, second):
        total = None
        for s in tiles(first.shape[1]):
            term = first[:, s] * second[:, s]
            total = term if total is None else total + term
        return total

    def send_row(sums):
        blocks = jnp.concatenate(sums + [jnp.zeros((LANES - pairs * len(sums), LANES), F32)], axis=0)
        turned = jnp.transpose(blocks)
        total = tree([two_sum(turned[i : i + 8], turned[i + 8 : i + 16]) for i in range(0, LANES, 16)], pair_add)
        for shift in (4, 2, 1):
            total = pair_add(total, tuple(pltpu.roll(x, shift, axis=0) for x in total))
        put_row(0, total)

    def put_row(stage, total):
        red[stage, 0, 0:1, :] = total[0][0:1]
        red[stage, 0, 1:2, :] = total[1][0:1]

    def reduction(stage, peers):
        for d, peer in peers:
            pltpu.make_async_remote_copy(
                src_ref=red.at[stage, 0],
                dst_ref=red.at[stage, d],
                send_sem=red_send.at[stage],
                recv_sem=red_recv.at[stage],
                device_id={"dom": peer},
                device_id_type=MESH,
            ).start()
        slots_used = red.at[stage, 1 : len(peers) + 1]
        return pltpu.make_async_remote_copy(
            src_ref=slots_used, dst_ref=slots_used, send_sem=red_send.at[stage], recv_sem=red_recv.at[stage],
            device_id={"dom": peers[0][1]}, device_id_type=MESH,
        )

    def summed(stage, count):
        return tree([(red[stage, d, 0:1, :], red[stage, d, 1:2, :]) for d in range(count)], pair_add)

    def spread_row(row):
        return jnp.transpose(jnp.broadcast_to(row, (LANES, LANES)))

    lhs[6 * pairs :, :] = jnp.zeros((pairs, nodes), BF16)
    loads[2].wait()
    for r in range(DIGITS):
        s = slice(r * words, (r + 1) * words)
        for i, piece in enumerate(pieces(cond[:, s] * scale_of(r))):
            lhs[6 * pairs + i : 6 * pairs + i + 1, s] = piece
        lhs[6 * pairs + 3 : 6 * pairs + 4, s] = jnp.full((1, words), scale_of(r), BF16)
    for s in tiles(nodes):
        split_part(cur[:, s], s)
    local_operator(cur, y0, True, u1, out1)
    ex1 = exchange(1, out1, in1)

    def remote_terms(u, other, t):
        for o in range(links):
            s = slice(o * LANES, (o + 1) * LANES)
            weight = jnp.concatenate([wsend[:, s]] * (pairs // 8), axis=0)
            t[:, s] = weight * (u[:, s] - other(o, s))

    ex0[0].wait_recv()
    ex0[1].wait_recv()
    for o in range(links):
        s = slice(o * LANES, (o + 1) * LANES)
        live = jnp.broadcast_to(send[o : o + 1, :], (8, LANES)) >= 0
        wsend[:, s] = jnp.where(live, half * (wsend[:, s] + in0[o, pairs : pairs + 1, :]), 0.0)
    remote_terms(u0, lambda o, s: in0[o, 0:pairs, :], t0)
    add_received(t0, y0, v1, True)
    local_operator(v1, y1, False, u2, out2)
    ex2 = exchange(2, out2, in2)
    moments = [lane_sums(cur, cur), lane_sums(cur, v1), lane_sums(v1, v1)]

    ex1[0].wait_recv()
    ex1[1].wait_recv()
    u1[...] = u1[...] + t0[...]
    remote_terms(u1, lambda o, s: in1[o, :, :] - t0[:, s], t1)
    add_received(t1, y1, v2, True)
    moments += [lane_sums(v1, v2), lane_sums(v2, v2)]
    local_operator(v2, y2, False)

    def last_terms(side):
        share = jnp.zeros((pairs, LANES), F32)
        for o in side:
            s = slice(o * LANES, (o + 1) * LANES)
            here = u2[:, s] + t1[:, s]
            apart = here - (in2[o, :, :] - t1[:, s])
            term = jnp.concatenate([wsend[:, s]] * (pairs // 8), axis=0) * apart
            t2[:, s] = term
            share = share + term * apart
        return share

    ex2[1].wait_recv()
    moments.append(lane_sums(v2, y2) + last_terms(range(reach, links)))
    send_row(moments)
    near_sums = reduction(0, near)

    ex2[0].wait_recv()
    last_terms(range(reach))
    add_received(t2, y2, v3, False)

    near_sums.wait_recv()
    put_row(1, summed(0, group))
    far_sums = reduction(1, far)
    far_sums.wait_recv()
    high, low = (spread_row(x) for x in summed(1, others))
    m = [(high[i * pairs : (i + 1) * pairs], low[i * pairs : (i + 1) * pairs]) for i in range(6)]

    m0 = m[0][0]
    a0, over_a0 = m0 / m[1][0], m[1][0] / m0
    square, square_rest = two_product(a0, a0)
    double = 2.0 * a0

    def shifted(i):
        p, p_rest = two_product(m[i + 1][0], double)
        q, q_rest = two_product(m[i + 2][0], square)
        p_rest = p_rest + m[i + 1][1] * double
        q_rest = q_rest + (m[i + 2][1] * square + m[i + 2][0] * square_rest)
        s, s_rest = two_sum(m[i][0], -p)
        s, t_rest = two_sum(s, q)
        return s + ((s_rest + t_rest) + (m[i][1] - p_rest + q_rest))

    k0, k1, k2, k3 = (shifted(i) for i in range(4))

    b1 = k0 / m0
    a1 = k0 / (k1 - b1 * k0 * over_a0)
    v1q1 = -(k0 * over_a0 + k1) * over_a0
    r2q1 = k1 - a1 * (k2 + b1 * v1q1)
    rr2 = -a1 * r2q1
    b2 = rr2 / k0
    v1q2 = (v1q1 - k2) * over_a0
    r2q2 = k2 - a1 * (k3 + b1 * v1q2)
    r2ar2 = r2q1 - a1 * (r2q2 - b1 * r2q1 * over_a0)
    a2 = rr2 / (r2ar2 + b2 * r2q1)

    for s in tiles(nodes):
        w0, w1, w2, w3 = cur[:, s], v1[:, s], v2[:, s], v3[:, s]
        r1 = w0 - a0 * w1
        q1 = w1 - a0 * w2
        q2 = w2 - a0 * w3
        p1 = r1 + b1 * w0
        ap1 = q1 + b1 * w1
        r2 = r1 - a1 * ap1
        ar2 = q1 - a1 * (q2 + b1 * w2)
        p2 = r2 + b2 * p1
        ap2 = ar2 + b2 * ap1
        volt[:, s] = a0 * w0 + a1 * p1 + a2 * p2
        resid[:, s] = r2 - a2 * ap2

    for copies in (*ex0, *ex1, *ex2, near_sums, far_sums):
        copies.wait_send()


def write_out(volt, resid, volt_out, resid_out, sems):
    copies = [pltpu.make_async_copy(volt, volt_out, sems.at[0]), pltpu.make_async_copy(resid, resid_out, sems.at[1])]
    for copy in copies:
        copy.start()
    for copy in copies:
        copy.wait()


def solve(parts, group, currents, conductance, ground, ell_cols, send_rows):
    pairs, nodes = currents.shape
    links = send_rows.shape[0]
    bound = links * LANES
    others = parts // group
    most = max(group, others)
    field = pltpu.VMEM((pairs, nodes), F32)
    edge = pltpu.VMEM((pairs, bound), F32)
    vmem = pl.BlockSpec(memory_space=pltpu.VMEM)
    volt, resid = pl.pallas_call(
        functools.partial(kernel, parts, group),
        out_shape=(jax.ShapeDtypeStruct((pairs, nodes), F32),) * 2,
        in_specs=[pl.BlockSpec(memory_space=pltpu.HBM)] * 5,
        out_specs=(vmem, vmem),
        scratch_shapes=[
            field,
            pltpu.VMEM((1, nodes), F32),
            pltpu.VMEM((1, nodes), F32),
            pltpu.VMEM(ell_cols.shape, I32),
            pltpu.VMEM(send_rows.shape, I32),
            pltpu.SemaphoreType.DMA((5,)),
            pltpu.VMEM((nodes // LANES, nodes, LANES), BF16),
            pltpu.VMEM((nodes // LANES, 1, LANES), I32),
            field, field, field, field, field, field,
            pltpu.VMEM((1, nodes), F32),
            pltpu.VMEM((7 * pairs, nodes), BF16),
            pltpu.VMEM((8, bound), F32),
            edge, edge, edge, edge, edge, edge,
            pltpu.VMEM((links, pairs + 1, LANES), F32),
            pltpu.VMEM((links, pairs, LANES), F32),
            pltpu.VMEM((links, pairs, LANES), F32),
            pltpu.VMEM((links, pairs + 1, LANES), F32),
            pltpu.VMEM((links, pairs, LANES), F32),
            pltpu.VMEM((links, pairs, LANES), F32),
            pltpu.VMEM((2, most, 2, LANES), F32),
            pltpu.SemaphoreType.DMA((3,)),
            pltpu.SemaphoreType.DMA((3, 2)),
            pltpu.SemaphoreType.DMA((2,)),
            pltpu.SemaphoreType.DMA((2,)),
        ],
        compiler_params=pltpu.CompilerParams(
            collective_id=0, has_side_effects=True, vmem_limit_bytes=48 * 1024 * 1024
        ),
    )(*(pltpu.with_memory_space_constraint(x, pltpu.HBM) for x in (currents, conductance.reshape(1, nodes), ground.reshape(1, nodes), ell_cols, send_rows)))
    return pl.pallas_call(
        write_out,
        out_shape=(jax.ShapeDtypeStruct((pairs, nodes), F32),) * 2,
        in_specs=[vmem] * 2,
        out_specs=(pl.BlockSpec(memory_space=pltpu.HBM),) * 2,
        scratch_shapes=[pltpu.SemaphoreType.DMA((2,))],
        compiler_params=pltpu.CompilerParams(vmem_limit_bytes=1 << 20),
    )(volt, resid)


def solution(mesh):
    parts = mesh.shape["dom"]
    group = 16 if parts >= 256 else 4
    placed = (P(None, "dom"), P("dom"), P("dom"), P(None, "dom"), P("dom", None))
    return jax.shard_map(
        functools.partial(solve, parts, group),
        mesh=mesh,
        in_specs=placed,
        out_specs=(P(None, "dom"), P(None, "dom")),
        check_vma=False,
    )
```

```python
import functools

import jax
import jax.numpy as jnp
from jax import lax
from jax.experimental import pallas as pl
from jax.experimental.pallas import tpu as pltpu
from jax.sharding import PartitionSpec as P

MESH = pl.DeviceIdType.MESH
F32, BF16, I32 = jnp.float32, jnp.bfloat16, jnp.int32
LANES = 128
WIDE = 256
DIGITS = 8


def pieces(x):
    high = x.astype(BF16)
    rest = x - high.astype(F32)
    mid = rest.astype(BF16)
    low = (rest - mid.astype(F32)).astype(BF16)
    return [high, mid, low]


def joined(y, first, rows):
    return (y[first + 2 * rows : first + 3 * rows] + y[first + rows : first + 2 * rows]) + y[first : first + rows]


def two_sum(a, b):
    s = a + b
    part = s - a
    return s, (a - (s - part)) + (b - part)


def two_product(a, b):
    p = a * b
    wide_a, wide_b = a * 4097.0, b * 4097.0
    a1 = wide_a - (wide_a - a)
    b1 = wide_b - (wide_b - b)
    a2, b2 = a - a1, b - b1
    return p, ((a1 * b1 - p) + a1 * b2 + a2 * b1) + a2 * b2


def pair_add(a, b):
    s, e = two_sum(a[0], b[0])
    e = e + (a[1] + b[1])
    high = s + e
    return high, e - (high - s)


def tree(terms, add):
    while len(terms) > 1:
        terms = [add(a, b) for a, b in zip(terms[0::2], terms[1::2], strict=True)]
    return terms[0]


def tiles(width):
    return [slice(i, i + LANES) for i in range(0, width, LANES)]


def kernel(
    parts, group, cur_in, cond_in, gnd_in, ell_in, send_in, volt, resid,
    cur, cond, gnd, ell, send, in_sem, adj, from_slot, v1, v2, v3, y0, y1, y2, diag, lhs, wsend, mat, tlhs, c_at, d_at, z_at, u0, u1, u2, t0, t1, t2,
    out0, out1, out2, in0, in1, in2, red, ex_send, ex_recv, red_send, red_recv,
):
    pairs, nodes = cur.shape
    slots = ell.shape[0]
    links = send.shape[0]
    bound = links * LANES
    reach = links // 2
    offsets = list(range(-reach, 0)) + list(range(1, reach + 1))
    me = lax.axis_index("dom")
    others = parts // group
    mine, place = me // group, me % group

    assert reach == 3
    neighbours, landing, side_of = [], [], []
    for o, e in enumerate(offsets):
        d = abs(e)
        edge = me if e < 0 else parts - 1 - me
        spare = jnp.where(edge == 0, 1 if d < 3 else 2, 0)
        spare_d = jnp.where(edge == 0, min(d + 1, 3), jnp.where(edge == 1, d - 1, 3))
        inside = edge >= d
        spare_peer = spare if e < 0 else parts - 1 - spare
        spare_slot = reach - spare_d if e < 0 else reach - 1 + spare_d
        neighbours.append(jnp.where(inside, me + e, spare_peer))
        landing.append(jnp.where(inside, links - 1 - o, spare_slot))
        side_of.append(jnp.where(inside, 1 if e < 0 else 0, 0 if e < 0 else 1))
    def steps(d, count):
        return min(d, count - d)

    near = [
        (d, mine * group + lax.rem(place + d, group))
        for d in sorted(range(1, group), key=lambda d: -steps(d, group))
    ]
    side = 4 if others == 16 else 2
    row, column = mine // side, mine % side
    far = [
        (d, (lax.rem(row + d // side, side) * side + lax.rem(column + d % side, side)) * group + place)
        for d in sorted(range(1, others), key=lambda d: -steps(d // side, side) - steps(d % side, side))
    ]

    loads = [
        pltpu.make_async_copy(source, target, in_sem.at[i])
        for i, (source, target) in enumerate(
            ((cur_in, cur), (cond_in, cond), (gnd_in, gnd), (ell_in, ell), (send_in, send))
        )
    ]
    loads[4].start()
    loads[0].start()
    for i in range(1, 4):
        loads[i].start()

    barrier = pltpu.get_barrier_semaphore()
    for peer in neighbours + [peer for _, peer in near + far]:
        pl.semaphore_signal(barrier, inc=1, device_id={"dom": peer}, device_id_type=MESH)
    word_ids = lax.broadcasted_iota(I32, (8, LANES), 0)
    no_word = jnp.zeros((8, LANES), I32)
    words = nodes // DIGITS

    def taken(x, lane):
        return jnp.take_along_axis(x, lane, axis=1, mode="promise_in_bounds")

    def places(o):
        node = jnp.broadcast_to(send[o : o + 1, :], (8, LANES))
        return node & (LANES - 1), lax.shift_right_arithmetic(node, 7)

    def picked(source, rows):
        found = []
        for o in range(links):
            lane, tile = places(o)
            parts_found = [jnp.zeros((8, LANES), F32)] * (rows // 8)
            for k, s in enumerate(tiles(nodes)):
                here = tile == k
                for i in range(rows // 8):
                    parts_found[i] = jnp.where(here, taken(source(i, s), lane), parts_found[i])
            found.append(jnp.concatenate(parts_found, axis=0))
        return found

    def field_rows(field):
        return lambda i, s: field[i * 8 : i * 8 + 8, s]

    with jax.named_scope("pick_cur"):
        loads[4].wait()
        loads[0].wait()
        loads[1].wait()
        for o, (u, c) in enumerate(
            zip(
                picked(field_rows(cur), pairs),
                picked(lambda i, s: jnp.broadcast_to(cond[:, s], (8, LANES)), 8),
                strict=True,
            )
        ):
            s = slice(o * LANES, (o + 1) * LANES)
            u0[:, s] = u
            wsend[:, s] = c
            c_at[:, s] = c
            out0[o, 0:pairs, :] = u
            out0[o, pairs : pairs + 1, :] = c[0:1]

    def send_all(step, out, into):
        for o in sorted(range(links), key=lambda o: -abs(offsets[o])):
            pltpu.make_async_remote_copy(
                src_ref=out.at[o],
                dst_ref=into.at[landing[o]],
                send_sem=ex_send.at[step],
                recv_sem=ex_recv.at[step, side_of[o]],
                device_id={"dom": neighbours[o]},
                device_id_type=MESH,
            ).start()

    def exchange(step, out, into):
        return [
            pltpu.make_async_remote_copy(
                src_ref=out.at[half], dst_ref=into.at[half], send_sem=ex_send.at[step], recv_sem=ex_recv.at[step, i],
                device_id={"dom": neighbours[0]}, device_id_type=MESH,
            )
            for i, half in enumerate((slice(0, reach), slice(reach, links)))
        ]

    def fill_counts(into, g, p, count, digits):
        word = list(p)
        for i in range(slots):
            for j in range(i):
                same = g[i] == g[j]
                word[i] = word[i] + jnp.where(same, p[j], no_word)
                word[j] = word[j] + jnp.where(same, p[i], no_word)
        for h in range(0, count, 64):
            chunk = []
            for q in range(h, h + 64, 8):
                ids = word_ids + q
                acc = no_word
                for s in range(slots):
                    acc = jnp.where(g[s] == ids, word[s], acc)
                chunk.append(acc)
            chunk = jnp.concatenate(chunk, axis=0)
            for r in range(digits):
                last = r == DIGITS - 1
                digit = lax.shift_right_logical(chunk, 4 * r) if last else chunk & (15 << (4 * r))
                into[r * count + h : r * count + h + 64, :] = digit.astype(F32).astype(BF16)

    def build(t, _):
        off = pl.multiple_of(t * LANES, LANES)
        block = ell[:, pl.ds(off, LANES)]
        local = (block >= 0) & (block < nodes)
        wide_g = jnp.where(local, block & (words - 1), -1)
        wide_p = jnp.left_shift(jnp.ones_like(block), jnp.where(local, (block // words) * 4, 0))
        g = [jnp.broadcast_to(wide_g[s : s + 1, :], (8, LANES)) for s in range(slots)]
        p = [jnp.broadcast_to(wide_p[s : s + 1, :], (8, LANES)) for s in range(slots)]
        fill_counts(adj.at[t], g, p, words, DIGITS)
        from_slot[t] = jnp.max(block, axis=0, keepdims=True) - nodes
        return 0

    def adj_block(b):
        return jnp.concatenate([adj[b // LANES], adj[b // LANES + 1]], axis=1)

    def scale_of(r):
        return 1.0 if r == DIGITS - 1 else 16.0**-r

    def split_part(value, s):
        part = value * scale_of(s.start // words)
        for i, piece in enumerate(pieces(part)):
            lhs[i * pairs : (i + 1) * pairs, s] = piece
        for i, piece in enumerate(pieces(part * cond[:, s])):
            lhs[(3 + i) * pairs : (4 + i) * pairs, s] = piece

    half = 0.5
    with jax.named_scope("adj_a"):
        loads[3].wait()
        ahead = jnp.where(place < group // 2, nodes // LANES, nodes // LANES * 7 // 16)
        lax.fori_loop(0, ahead, build, 0)
    with jax.named_scope("barwait"):
        pl.semaphore_wait(barrier, len(neighbours) + len(near) + len(far))
    send_all(0, out0, in0)
    ex0 = exchange(0, out0, in0)
    with jax.named_scope("adj_b"):
        lax.fori_loop(ahead, nodes // LANES, build, 0)

    def local_operator(v, y, first, u=None, out=None):
        if u is not None:
            listed = [places(o) for o in range(links)]
            found = [[jnp.zeros((8, LANES), F32)] * (pairs // 8) for _ in range(links)]
        rows = 7 * pairs if first else 6 * pairs
        for b in range(0, nodes, WIDE):
            s = slice(b, b + WIDE)
            prod = jnp.dot(lhs[0:rows, :], adj_block(b), preferred_element_type=F32)
            c = cond[:, s]
            if first:
                extra = prod[6 * pairs :]
                around = joined(extra, 0, 1)
                diag[:, s] = gnd[:, s] + half * (c * extra[3:4] + around)
            result = diag[:, s] * v[:, s] - half * (c * joined(prod, 0, pairs) + joined(prod, 3 * pairs, pairs))
            y[:, s] = result
            if u is not None:
                for k in (b // LANES, b // LANES + 1):
                    inner = k * LANES - b
                    for o, (lane, tile) in enumerate(listed):
                        here = tile == k
                        for i in range(pairs // 8):
                            piece = result[i * 8 : i * 8 + 8, inner : inner + LANES]
                            found[o][i] = jnp.where(here, taken(piece, lane), found[o][i])
        if u is not None:
            for o in range(links):
                both = jnp.concatenate(found[o], axis=0)
                u[:, o * LANES : (o + 1) * LANES] = both
                if out is not None:
                    out[o, :, :] = both

    def add_received(t, y, v, onward):
        for k, s in enumerate(tiles(nodes)):
            slot = jnp.broadcast_to(from_slot[k], (8, LANES))
            lane, link = slot & (LANES - 1), lax.shift_right_arithmetic(slot, 7)
            found = [jnp.zeros((8, LANES), F32)] * (pairs // 8)
            for o, part in enumerate(tiles(bound)):
                here = link == o
                for i in range(pairs // 8):
                    found[i] = jnp.where(here, taken(t[i * 8 : i * 8 + 8, part], lane), found[i])
            value = y[:, s] + jnp.concatenate(found, axis=0)
            v[:, s] = value
            if onward:
                split_part(value, s)

    def lane_sums(first, second):
        total = None
        for s in tiles(first.shape[1]):
            term = first[:, s] * second[:, s]
            total = term if total is None else total + term
        return total

    def send_row(sums):
        blocks = jnp.concatenate(sums + [jnp.zeros((LANES - pairs * len(sums), LANES), F32)], axis=0)
        turned = jnp.transpose(blocks)
        total = tree([two_sum(turned[i : i + 8], turned[i + 8 : i + 16]) for i in range(0, LANES, 16)], pair_add)
        for shift in (4, 2, 1):
            total = pair_add(total, tuple(pltpu.roll(x, shift, axis=0) for x in total))
        put_row(0, total)

    def put_row(stage, total):
        red[stage, 0, 0:1, :] = total[0][0:1]
        red[stage, 0, 1:2, :] = total[1][0:1]

    def reduction(stage, peers):
        for d, peer in peers:
            pltpu.make_async_remote_copy(
                src_ref=red.at[stage, 0],
                dst_ref=red.at[stage, d],
                send_sem=red_send.at[stage],
                recv_sem=red_recv.at[stage],
                device_id={"dom": peer},
                device_id_type=MESH,
            ).start()
        slots_used = red.at[stage, 1 : len(peers) + 1]
        return pltpu.make_async_remote_copy(
            src_ref=slots_used, dst_ref=slots_used, send_sem=red_send.at[stage], recv_sem=red_recv.at[stage],
            device_id={"dom": peers[0][1]}, device_id_type=MESH,
        )

    def summed(stage, count):
        return tree([(red[stage, d, 0:1, :], red[stage, d, 1:2, :]) for d in range(count)], pair_add)

    def spread_row(row):
        return jnp.transpose(jnp.broadcast_to(row, (LANES, LANES)))

    lhs[6 * pairs :, :] = jnp.zeros((pairs, nodes), BF16)
    loads[2].wait()
    for r in range(DIGITS):
        s = slice(r * words, (r + 1) * words)
        for i, piece in enumerate(pieces(cond[:, s] * scale_of(r))):
            lhs[6 * pairs + i : 6 * pairs + i + 1, s] = piece
        lhs[6 * pairs + 3 : 6 * pairs + 4, s] = jnp.full((1, words), scale_of(r), BF16)
    for s in tiles(nodes):
        split_part(cur[:, s], s)
    local_operator(cur, y0, True, u1, out1)
    send_all(1, out1, in1)
    ex1 = exchange(1, out1, in1)

    def remote_terms(u, other, t):
        for o in range(links):
            s = slice(o * LANES, (o + 1) * LANES)
            weight = jnp.concatenate([wsend[:, s]] * (pairs // 8), axis=0)
            t[:, s] = weight * (u[:, s] - other(o, s))

    early = place < 4

    @pl.when(early)
    def _():
        with jax.named_scope("prep"):
            for o, d in enumerate(picked(lambda i, s: jnp.broadcast_to(diag[:, s], (8, LANES)), 8)):
                d_at[:, o * LANES : (o + 1) * LANES] = d
            for s in tiles(nodes):
                split_part(y0[:, s], s)
            local_operator(y0, y1, False, z_at)
            spans = [(0, 8)] + [(i, i + 1) for i in range(8, slots)]
            for o in range(links):
                lane, tile = places(o)
                g, p = [], []
                for first, end in spans:
                    near_by = jnp.full((8, LANES), -1, I32)
                    for k, s in enumerate(tiles(nodes)):
                        rows = jnp.broadcast_to(ell[first:end, s], (8, LANES))
                        near_by = jnp.where(tile == k, taken(rows, lane), near_by)
                    inner = near_by & (LANES - 1)
                    outer = jnp.where(near_by < nodes, lax.shift_right_arithmetic(near_by, 7), -1)
                    slot = jnp.full((8, LANES), -1, I32)
                    for k in range(nodes // LANES):
                        known = jnp.broadcast_to(from_slot[k], (8, LANES))
                        slot = jnp.where(outer == k, taken(known, inner), slot)
                    word = jnp.where(slot >= 0, slot & (LANES - 1), -1)
                    power = jnp.left_shift(
                        jnp.ones_like(slot), jnp.where(slot >= 0, lax.shift_right_arithmetic(slot, 7) * 4, 0)
                    )
                    for i in range(end - first):
                        g.append(jnp.broadcast_to(word[i : i + 1], (8, LANES)))
                        p.append(jnp.broadcast_to(power[i : i + 1], (8, LANES)))
                fill_counts(mat.at[o], g, p, LANES, links)

    ex0[0].wait_recv()
    ex0[1].wait_recv()
    for o in range(links):
        s = slice(o * LANES, (o + 1) * LANES)
        live = jnp.broadcast_to(send[o : o + 1, :], (8, LANES)) >= 0
        wsend[:, s] = jnp.where(live, half * (wsend[:, s] + in0[o, pairs : pairs + 1, :]), 0.0)
    remote_terms(u0, lambda o, s: in0[o, 0:pairs, :], t0)
    def both_halves(x):
        return jnp.concatenate([x] * (pairs // 8), axis=0)

    @pl.when(early)
    def _():
        with jax.named_scope("short"):
            for r, s in enumerate(tiles(bound)):
                part = t0[:, s] * 16.0**-r
                for i, piece in enumerate(pieces(part)):
                    tlhs[i * pairs : (i + 1) * pairs, s] = piece
                for i, piece in enumerate(pieces(part * both_halves(c_at[:, s]))):
                    tlhs[(3 + i) * pairs : (4 + i) * pairs, s] = piece
            for b in range(0, bound, WIDE):
                counts = jnp.concatenate([mat[b // LANES], mat[b // LANES + 1]], axis=1)
                prod = jnp.dot(tlhs[...], counts, preferred_element_type=F32)
                for o in (b // LANES, b // LANES + 1):
                    s = slice(o * LANES, (o + 1) * LANES)
                    half_prod = prod[:, o * LANES - b : (o + 1) * LANES - b]
                    around = both_halves(c_at[:, s]) * joined(half_prod, 0, pairs)
                    around = around + joined(half_prod, 3 * pairs, pairs)
                    value = z_at[:, s] + (both_halves(d_at[:, s]) * t0[:, s] - half * around)
                    u2[:, s] = value
                    out2[o, :, :] = value
            send_all(2, out2, in2)

    add_received(t0, y0, v1, True)

    @pl.when(early)
    def _():
        local_operator(v1, y1, False)

    @pl.when(jnp.logical_not(early))
    def _():
        local_operator(v1, y1, False, u2, out2)
        send_all(2, out2, in2)

    ex2 = exchange(2, out2, in2)
    moments = [lane_sums(cur, cur), lane_sums(cur, v1), lane_sums(v1, v1)]

    ex1[0].wait_recv()
    ex1[1].wait_recv()
    u1[...] = u1[...] + t0[...]
    remote_terms(u1, lambda o, s: in1[o, :, :] - t0[:, s], t1)
    add_received(t1, y1, v2, True)
    moments += [lane_sums(v1, v2), lane_sums(v2, v2)]
    local_operator(v2, y2, False)

    def last_terms(side):
        share = jnp.zeros((pairs, LANES), F32)
        for o in side:
            s = slice(o * LANES, (o + 1) * LANES)
            here = u2[:, s] + t1[:, s]
            apart = here - (in2[o, :, :] - t1[:, s])
            term = jnp.concatenate([wsend[:, s]] * (pairs // 8), axis=0) * apart
            t2[:, s] = term
            share = share + term * apart
        return share

    ex2[1].wait_recv()
    moments.append(lane_sums(v2, y2) + last_terms(range(reach, links)))
    send_row(moments)
    near_sums = reduction(0, near)

    ex2[0].wait_recv()
    last_terms(range(reach))
    add_received(t2, y2, v3, False)

    near_sums.wait_recv()
    put_row(1, summed(0, group))
    far_sums = reduction(1, far)
    far_sums.wait_recv()
    high, low = (spread_row(x) for x in summed(1, others))
    m = [(high[i * pairs : (i + 1) * pairs], low[i * pairs : (i + 1) * pairs]) for i in range(6)]

    m0 = m[0][0]
    a0, over_a0 = m0 / m[1][0], m[1][0] / m0
    square, square_rest = two_product(a0, a0)
    double = 2.0 * a0

    def shifted(i):
        p, p_rest = two_product(m[i + 1][0], double)
        q, q_rest = two_product(m[i + 2][0], square)
        p_rest = p_rest + m[i + 1][1] * double
        q_rest = q_rest + (m[i + 2][1] * square + m[i + 2][0] * square_rest)
        s, s_rest = two_sum(m[i][0], -p)
        s, t_rest = two_sum(s, q)
        return s + ((s_rest + t_rest) + (m[i][1] - p_rest + q_rest))

    k0, k1, k2, k3 = (shifted(i) for i in range(4))

    b1 = k0 / m0
    a1 = k0 / (k1 - b1 * k0 * over_a0)
    v1q1 = -(k0 * over_a0 + k1) * over_a0
    r2q1 = k1 - a1 * (k2 + b1 * v1q1)
    rr2 = -a1 * r2q1
    b2 = rr2 / k0
    v1q2 = (v1q1 - k2) * over_a0
    r2q2 = k2 - a1 * (k3 + b1 * v1q2)
    r2ar2 = r2q1 - a1 * (r2q2 - b1 * r2q1 * over_a0)
    a2 = rr2 / (r2ar2 + b2 * r2q1)

    for s in tiles(nodes):
        w0, w1, w2, w3 = cur[:, s], v1[:, s], v2[:, s], v3[:, s]
        r1 = w0 - a0 * w1
        q1 = w1 - a0 * w2
        q2 = w2 - a0 * w3
        p1 = r1 + b1 * w0
        ap1 = q1 + b1 * w1
        r2 = r1 - a1 * ap1
        ar2 = q1 - a1 * (q2 + b1 * w2)
        p2 = r2 + b2 * p1
        ap2 = ar2 + b2 * ap1
        volt[:, s] = a0 * w0 + a1 * p1 + a2 * p2
        resid[:, s] = r2 - a2 * ap2

    for copies in (*ex0, *ex1, *ex2, near_sums, far_sums):
        copies.wait_send()


def write_out(volt, resid, volt_out, resid_out, sems):
    copies = [pltpu.make_async_copy(volt, volt_out, sems.at[0]), pltpu.make_async_copy(resid, resid_out, sems.at[1])]
    for copy in copies:
        copy.start()
    for copy in copies:
        copy.wait()


def solve(parts, group, currents, conductance, ground, ell_cols, send_rows):
    pairs, nodes = currents.shape
    links = send_rows.shape[0]
    bound = links * LANES
    others = parts // group
    most = max(group, others)
    field = pltpu.VMEM((pairs, nodes), F32)
    edge = pltpu.VMEM((pairs, bound), F32)
    vmem = pl.BlockSpec(memory_space=pltpu.VMEM)
    volt, resid = pl.pallas_call(
        functools.partial(kernel, parts, group),
        out_shape=(jax.ShapeDtypeStruct((pairs, nodes), F32),) * 2,
        in_specs=[pl.BlockSpec(memory_space=pltpu.HBM)] * 5,
        out_specs=(vmem, vmem),
        scratch_shapes=[
            field,
            pltpu.VMEM((1, nodes), F32),
            pltpu.VMEM((1, nodes), F32),
            pltpu.VMEM(ell_cols.shape, I32),
            pltpu.VMEM(send_rows.shape, I32),
            pltpu.SemaphoreType.DMA((5,)),
            pltpu.VMEM((nodes // LANES, nodes, LANES), BF16),
            pltpu.VMEM((nodes // LANES, 1, LANES), I32),
            field, field, field, field, field, field,
            pltpu.VMEM((1, nodes), F32),
            pltpu.VMEM((7 * pairs, nodes), BF16),
            pltpu.VMEM((8, bound), F32),
            pltpu.VMEM((links, bound, LANES), BF16),
            pltpu.VMEM((6 * pairs, bound), BF16),
            pltpu.VMEM((8, bound), F32),
            pltpu.VMEM((8, bound), F32),
            edge,
            edge, edge, edge, edge, edge, edge,
            pltpu.VMEM((links, pairs + 1, LANES), F32),
            pltpu.VMEM((links, pairs, LANES), F32),
            pltpu.VMEM((links, pairs, LANES), F32),
            pltpu.VMEM((links, pairs + 1, LANES), F32),
            pltpu.VMEM((links, pairs, LANES), F32),
            pltpu.VMEM((links, pairs, LANES), F32),
            pltpu.VMEM((2, most, 2, LANES), F32),
            pltpu.SemaphoreType.DMA((3,)),
            pltpu.SemaphoreType.DMA((3, 2)),
            pltpu.SemaphoreType.DMA((2,)),
            pltpu.SemaphoreType.DMA((2,)),
        ],
        compiler_params=pltpu.CompilerParams(
            collective_id=0, has_side_effects=True, vmem_limit_bytes=48 * 1024 * 1024
        ),
    )(*(pltpu.with_memory_space_constraint(x, pltpu.HBM) for x in (currents, conductance.reshape(1, nodes), ground.reshape(1, nodes), ell_cols, send_rows)))
    return pl.pallas_call(
        write_out,
        out_shape=(jax.ShapeDtypeStruct((pairs, nodes), F32),) * 2,
        in_specs=[vmem] * 2,
        out_specs=(pl.BlockSpec(memory_space=pltpu.HBM),) * 2,
        scratch_shapes=[pltpu.SemaphoreType.DMA((2,))],
        compiler_params=pltpu.CompilerParams(vmem_limit_bytes=1 << 20),
    )(volt, resid)


def solution(mesh):
    parts = mesh.shape["dom"]
    group = 16 if parts >= 256 else 4
    placed = (P(None, "dom"), P("dom"), P("dom"), P(None, "dom"), P("dom", None))
    return jax.shard_map(
        functools.partial(solve, parts, group),
        mesh=mesh,
        in_specs=placed,
        out_specs=(P(None, "dom"), P(None, "dom")),
        check_vma=False,
    )
```

```python
import functools

import jax
import jax.numpy as jnp
from jax import lax
from jax.experimental import pallas as pl
from jax.experimental.pallas import tpu as pltpu
from jax.sharding import PartitionSpec as P

MESH = pl.DeviceIdType.MESH
F32, BF16, I32 = jnp.float32, jnp.bfloat16, jnp.int32
LANES = 128
WIDE = 256
DIGITS = 8


def pieces(x):
    high = x.astype(BF16)
    rest = x - high.astype(F32)
    mid = rest.astype(BF16)
    low = (rest - mid.astype(F32)).astype(BF16)
    return [high, mid, low]


def joined(y, first, rows):
    return (y[first + 2 * rows : first + 3 * rows] + y[first + rows : first + 2 * rows]) + y[first : first + rows]


def two_sum(a, b):
    s = a + b
    part = s - a
    return s, (a - (s - part)) + (b - part)


def two_product(a, b):
    p = a * b
    wide_a, wide_b = a * 4097.0, b * 4097.0
    a1 = wide_a - (wide_a - a)
    b1 = wide_b - (wide_b - b)
    a2, b2 = a - a1, b - b1
    return p, ((a1 * b1 - p) + a1 * b2 + a2 * b1) + a2 * b2


def pair_add(a, b):
    s, e = two_sum(a[0], b[0])
    e = e + (a[1] + b[1])
    high = s + e
    return high, e - (high - s)


def tree(terms, add):
    while len(terms) > 1:
        terms = [add(a, b) for a, b in zip(terms[0::2], terms[1::2], strict=True)]
    return terms[0]


def tiles(width):
    return [slice(i, i + LANES) for i in range(0, width, LANES)]


def kernel(
    parts, group, cur_in, cond_in, gnd_in, ell_in, send_in, volt, resid,
    cur, cond, gnd, ell, send, in_sem, adj, from_slot, v1, v2, v3, y0, y1, y2, diag, lhs, wsend, mat, tlhs, c_at, d_at, z_at, u0, u1, u2, t0, t1, t2,
    out0, out1, out2, in0, in1, in2, red, ex_send, ex_recv, red_send, red_recv,
):
    pairs, nodes = cur.shape
    slots = ell.shape[0]
    links = send.shape[0]
    bound = links * LANES
    reach = links // 2
    offsets = list(range(-reach, 0)) + list(range(1, reach + 1))
    me = lax.axis_index("dom")
    others = parts // group
    mine, place = me // group, me % group

    assert reach == 3
    neighbours, landing, side_of = [], [], []
    for o, e in enumerate(offsets):
        d = abs(e)
        edge = me if e < 0 else parts - 1 - me
        spare = jnp.where(edge == 0, 1 if d < 3 else 2, 0)
        spare_d = jnp.where(edge == 0, min(d + 1, 3), jnp.where(edge == 1, d - 1, 3))
        inside = edge >= d
        spare_peer = spare if e < 0 else parts - 1 - spare
        spare_slot = reach - spare_d if e < 0 else reach - 1 + spare_d
        neighbours.append(jnp.where(inside, me + e, spare_peer))
        landing.append(jnp.where(inside, links - 1 - o, spare_slot))
        side_of.append(jnp.where(inside, 1 if e < 0 else 0, 0 if e < 0 else 1))
    def steps(d, count):
        return min(d, count - d)

    near = [
        (d, mine * group + lax.rem(place + d, group))
        for d in sorted(range(1, group), key=lambda d: -steps(d, group))
    ]
    side = 4 if others == 16 else 2
    row, column = mine // side, mine % side
    far = [
        (d, (lax.rem(row + d // side, side) * side + lax.rem(column + d % side, side)) * group + place)
        for d in sorted(range(1, others), key=lambda d: -steps(d // side, side) - steps(d % side, side))
    ]

    loads = [
        pltpu.make_async_copy(source, target, in_sem.at[i])
        for i, (source, target) in enumerate(
            ((cur_in, cur), (cond_in, cond), (gnd_in, gnd), (ell_in, ell), (send_in, send))
        )
    ]
    loads[4].start()
    loads[0].start()
    for i in range(1, 4):
        loads[i].start()

    barrier = pltpu.get_barrier_semaphore()
    for peer in neighbours + [peer for _, peer in near + far]:
        pl.semaphore_signal(barrier, inc=1, device_id={"dom": peer}, device_id_type=MESH)
    word_ids = lax.broadcasted_iota(I32, (8, LANES), 0)
    no_word = jnp.zeros((8, LANES), I32)
    words = nodes // DIGITS

    def taken(x, lane):
        return jnp.take_along_axis(x, lane, axis=1, mode="promise_in_bounds")

    def places(o):
        node = jnp.broadcast_to(send[o : o + 1, :], (8, LANES))
        return node & (LANES - 1), lax.shift_right_arithmetic(node, 7)

    def picked(source, rows):
        found = []
        for o in range(links):
            lane, tile = places(o)
            parts_found = [jnp.zeros((8, LANES), F32)] * (rows // 8)
            for k, s in enumerate(tiles(nodes)):
                here = tile == k
                for i in range(rows // 8):
                    parts_found[i] = jnp.where(here, taken(source(i, s), lane), parts_found[i])
            found.append(jnp.concatenate(parts_found, axis=0))
        return found

    def field_rows(field):
        return lambda i, s: field[i * 8 : i * 8 + 8, s]

    with jax.named_scope("pick_cur"):
        loads[4].wait()
        loads[0].wait()
        loads[1].wait()
        for o, (u, c) in enumerate(
            zip(
                picked(field_rows(cur), pairs),
                picked(lambda i, s: jnp.broadcast_to(cond[:, s], (8, LANES)), 8),
                strict=True,
            )
        ):
            s = slice(o * LANES, (o + 1) * LANES)
            u0[:, s] = u
            wsend[:, s] = c
            c_at[:, s] = c
            out0[o, 0:pairs, :] = u
            out0[o, pairs : pairs + 1, :] = c[0:1]

    def send_all(step, out, into):
        for o in sorted(range(links), key=lambda o: -abs(offsets[o])):
            pltpu.make_async_remote_copy(
                src_ref=out.at[o],
                dst_ref=into.at[landing[o]],
                send_sem=ex_send.at[step],
                recv_sem=ex_recv.at[step, side_of[o]],
                device_id={"dom": neighbours[o]},
                device_id_type=MESH,
            ).start()

    def exchange(step, out, into):
        return [
            pltpu.make_async_remote_copy(
                src_ref=out.at[half], dst_ref=into.at[half], send_sem=ex_send.at[step], recv_sem=ex_recv.at[step, i],
                device_id={"dom": neighbours[0]}, device_id_type=MESH,
            )
            for i, half in enumerate((slice(0, reach), slice(reach, links)))
        ]

    def fill_counts(into, g, p, count, digits):
        word = list(p)
        for i in range(slots):
            for j in range(i):
                same = g[i] == g[j]
                word[i] = word[i] + jnp.where(same, p[j], no_word)
                word[j] = word[j] + jnp.where(same, p[i], no_word)
        for h in range(0, count, 64):
            chunk = []
            for q in range(h, h + 64, 8):
                ids = word_ids + q
                acc = no_word
                for s in range(slots):
                    acc = jnp.where(g[s] == ids, word[s], acc)
                chunk.append(acc)
            chunk = jnp.concatenate(chunk, axis=0)
            for r in range(digits):
                last = r == DIGITS - 1
                digit = lax.shift_right_logical(chunk, 4 * r) if last else chunk & (15 << (4 * r))
                into[r * count + h : r * count + h + 64, :] = digit.astype(F32).astype(BF16)

    def build(t, _):
        off = pl.multiple_of(t * LANES, LANES)
        block = ell[:, pl.ds(off, LANES)]
        local = (block >= 0) & (block < nodes)
        wide_g = jnp.where(local, block & (words - 1), -1)
        wide_p = jnp.left_shift(jnp.ones_like(block), jnp.where(local, (block // words) * 4, 0))
        g = [jnp.broadcast_to(wide_g[s : s + 1, :], (8, LANES)) for s in range(slots)]
        p = [jnp.broadcast_to(wide_p[s : s + 1, :], (8, LANES)) for s in range(slots)]
        fill_counts(adj.at[t], g, p, words, DIGITS)
        from_slot[t] = jnp.max(block, axis=0, keepdims=True) - nodes
        return 0

    def adj_block(b):
        return jnp.concatenate([adj[b // LANES], adj[b // LANES + 1]], axis=1)

    def scale_of(r):
        return 1.0 if r == DIGITS - 1 else 16.0**-r

    def split_part(value, s):
        part = value * scale_of(s.start // words)
        for i, piece in enumerate(pieces(part)):
            lhs[i * pairs : (i + 1) * pairs, s] = piece
        for i, piece in enumerate(pieces(part * cond[:, s])):
            lhs[(3 + i) * pairs : (4 + i) * pairs, s] = piece

    half = 0.5
    with jax.named_scope("adj_a"):
        loads[3].wait()
        part_of = jnp.where(row == 0, 16, jnp.where(row == 1, 10, 4))
        ahead = jnp.where(place < group // 2, nodes // LANES, nodes // LANES * part_of // 16)
        lax.fori_loop(0, ahead, build, 0)
    with jax.named_scope("barwait"):
        pl.semaphore_wait(barrier, len(neighbours) + len(near) + len(far))
    send_all(0, out0, in0)
    ex0 = exchange(0, out0, in0)
    with jax.named_scope("adj_b"):
        lax.fori_loop(ahead, nodes // LANES, build, 0)

    def local_operator(v, y, first, u=None, out=None):
        if u is not None:
            listed = [places(o) for o in range(links)]
            found = [[jnp.zeros((8, LANES), F32)] * (pairs // 8) for _ in range(links)]
        rows = 7 * pairs if first else 6 * pairs
        for b in range(0, nodes, WIDE):
            s = slice(b, b + WIDE)
            prod = jnp.dot(lhs[0:rows, :], adj_block(b), preferred_element_type=F32)
            c = cond[:, s]
            if first:
                extra = prod[6 * pairs :]
                around = joined(extra, 0, 1)
                diag[:, s] = gnd[:, s] + half * (c * extra[3:4] + around)
            result = diag[:, s] * v[:, s] - half * (c * joined(prod, 0, pairs) + joined(prod, 3 * pairs, pairs))
            y[:, s] = result
            if u is not None:
                for k in (b // LANES, b // LANES + 1):
                    inner = k * LANES - b
                    for o, (lane, tile) in enumerate(listed):
                        here = tile == k
                        for i in range(pairs // 8):
                            piece = result[i * 8 : i * 8 + 8, inner : inner + LANES]
                            found[o][i] = jnp.where(here, taken(piece, lane), found[o][i])
        if u is not None:
            for o in range(links):
                both = jnp.concatenate(found[o], axis=0)
                u[:, o * LANES : (o + 1) * LANES] = both
                if out is not None:
                    out[o, :, :] = both

    def add_received(t, y, v, onward):
        for k, s in enumerate(tiles(nodes)):
            slot = jnp.broadcast_to(from_slot[k], (8, LANES))
            lane, link = slot & (LANES - 1), lax.shift_right_arithmetic(slot, 7)
            found = [jnp.zeros((8, LANES), F32)] * (pairs // 8)
            for o, part in enumerate(tiles(bound)):
                here = link == o
                for i in range(pairs // 8):
                    found[i] = jnp.where(here, taken(t[i * 8 : i * 8 + 8, part], lane), found[i])
            value = y[:, s] + jnp.concatenate(found, axis=0)
            v[:, s] = value
            if onward:
                split_part(value, s)

    def lane_sums(first, second):
        total = None
        for s in tiles(first.shape[1]):
            term = first[:, s] * second[:, s]
            total = term if total is None else total + term
        return total

    def send_row(sums):
        blocks = jnp.concatenate(sums + [jnp.zeros((LANES - pairs * len(sums), LANES), F32)], axis=0)
        turned = jnp.transpose(blocks)
        total = tree([two_sum(turned[i : i + 8], turned[i + 8 : i + 16]) for i in range(0, LANES, 16)], pair_add)
        for shift in (4, 2, 1):
            total = pair_add(total, tuple(pltpu.roll(x, shift, axis=0) for x in total))
        put_row(0, total)

    def put_row(stage, total):
        red[stage, 0, 0:1, :] = total[0][0:1]
        red[stage, 0, 1:2, :] = total[1][0:1]

    def reduction(stage, peers):
        for d, peer in peers:
            pltpu.make_async_remote_copy(
                src_ref=red.at[stage, 0],
                dst_ref=red.at[stage, d],
                send_sem=red_send.at[stage],
                recv_sem=red_recv.at[stage],
                device_id={"dom": peer},
                device_id_type=MESH,
            ).start()
        slots_used = red.at[stage, 1 : len(peers) + 1]
        return pltpu.make_async_remote_copy(
            src_ref=slots_used, dst_ref=slots_used, send_sem=red_send.at[stage], recv_sem=red_recv.at[stage],
            device_id={"dom": peers[0][1]}, device_id_type=MESH,
        )

    def summed(stage, count):
        return tree([(red[stage, d, 0:1, :], red[stage, d, 1:2, :]) for d in range(count)], pair_add)

    def spread_row(row):
        return jnp.transpose(jnp.broadcast_to(row, (LANES, LANES)))

    lhs[6 * pairs :, :] = jnp.zeros((pairs, nodes), BF16)
    loads[2].wait()
    for r in range(DIGITS):
        s = slice(r * words, (r + 1) * words)
        for i, piece in enumerate(pieces(cond[:, s] * scale_of(r))):
            lhs[6 * pairs + i : 6 * pairs + i + 1, s] = piece
        lhs[6 * pairs + 3 : 6 * pairs + 4, s] = jnp.full((1, words), scale_of(r), BF16)
    for s in tiles(nodes):
        split_part(cur[:, s], s)
    local_operator(cur, y0, True, u1, out1)
    send_all(1, out1, in1)
    ex1 = exchange(1, out1, in1)

    def remote_terms(u, other, t):
        for o in range(links):
            s = slice(o * LANES, (o + 1) * LANES)
            weight = jnp.concatenate([wsend[:, s]] * (pairs // 8), axis=0)
            t[:, s] = weight * (u[:, s] - other(o, s))

    early = place < 4

    @pl.when(early)
    def _():
        with jax.named_scope("prep"):
            for o, d in enumerate(picked(lambda i, s: jnp.broadcast_to(diag[:, s], (8, LANES)), 8)):
                d_at[:, o * LANES : (o + 1) * LANES] = d
            for s in tiles(nodes):
                split_part(y0[:, s], s)
            local_operator(y0, y1, False, z_at)
            spans = [(0, 8)] + [(i, i + 1) for i in range(8, slots)]
            for o in range(links):
                lane, tile = places(o)
                g, p = [], []
                for first, end in spans:
                    near_by = jnp.full((8, LANES), -1, I32)
                    for k, s in enumerate(tiles(nodes)):
                        rows = jnp.broadcast_to(ell[first:end, s], (8, LANES))
                        near_by = jnp.where(tile == k, taken(rows, lane), near_by)
                    inner = near_by & (LANES - 1)
                    outer = jnp.where(near_by < nodes, lax.shift_right_arithmetic(near_by, 7), -1)
                    slot = jnp.full((8, LANES), -1, I32)
                    for k in range(nodes // LANES):
                        known = jnp.broadcast_to(from_slot[k], (8, LANES))
                        slot = jnp.where(outer == k, taken(known, inner), slot)
                    word = jnp.where(slot >= 0, slot & (LANES - 1), -1)
                    power = jnp.left_shift(
                        jnp.ones_like(slot), jnp.where(slot >= 0, lax.shift_right_arithmetic(slot, 7) * 4, 0)
                    )
                    for i in range(end - first):
                        g.append(jnp.broadcast_to(word[i : i + 1], (8, LANES)))
                        p.append(jnp.broadcast_to(power[i : i + 1], (8, LANES)))
                fill_counts(mat.at[o], g, p, LANES, links)

    ex0[0].wait_recv()
    ex0[1].wait_recv()
    for o in range(links):
        s = slice(o * LANES, (o + 1) * LANES)
        live = jnp.broadcast_to(send[o : o + 1, :], (8, LANES)) >= 0
        wsend[:, s] = jnp.where(live, half * (wsend[:, s] + in0[o, pairs : pairs + 1, :]), 0.0)
    remote_terms(u0, lambda o, s: in0[o, 0:pairs, :], t0)
    def both_halves(x):
        return jnp.concatenate([x] * (pairs // 8), axis=0)

    @pl.when(early)
    def _():
        with jax.named_scope("short"):
            for r, s in enumerate(tiles(bound)):
                part = t0[:, s] * 16.0**-r
                for i, piece in enumerate(pieces(part)):
                    tlhs[i * pairs : (i + 1) * pairs, s] = piece
                for i, piece in enumerate(pieces(part * both_halves(c_at[:, s]))):
                    tlhs[(3 + i) * pairs : (4 + i) * pairs, s] = piece
            for b in range(0, bound, WIDE):
                counts = jnp.concatenate([mat[b // LANES], mat[b // LANES + 1]], axis=1)
                prod = jnp.dot(tlhs[...], counts, preferred_element_type=F32)
                for o in (b // LANES, b // LANES + 1):
                    s = slice(o * LANES, (o + 1) * LANES)
                    half_prod = prod[:, o * LANES - b : (o + 1) * LANES - b]
                    around = both_halves(c_at[:, s]) * joined(half_prod, 0, pairs)
                    around = around + joined(half_prod, 3 * pairs, pairs)
                    value = z_at[:, s] + (both_halves(d_at[:, s]) * t0[:, s] - half * around)
                    u2[:, s] = value
                    out2[o, :, :] = value
            send_all(2, out2, in2)

    add_received(t0, y0, v1, True)

    @pl.when(early)
    def _():
        local_operator(v1, y1, False)

    @pl.when(jnp.logical_not(early))
    def _():
        local_operator(v1, y1, False, u2, out2)
        send_all(2, out2, in2)

    ex2 = exchange(2, out2, in2)
    moments = [lane_sums(cur, cur), lane_sums(cur, v1), lane_sums(v1, v1)]

    ex1[0].wait_recv()
    ex1[1].wait_recv()
    u1[...] = u1[...] + t0[...]
    remote_terms(u1, lambda o, s: in1[o, :, :] - t0[:, s], t1)
    add_received(t1, y1, v2, True)
    moments += [lane_sums(v1, v2), lane_sums(v2, v2)]
    local_operator(v2, y2, False)

    def last_terms(side):
        share = jnp.zeros((pairs, LANES), F32)
        for o in side:
            s = slice(o * LANES, (o + 1) * LANES)
            here = u2[:, s] + t1[:, s]
            apart = here - (in2[o, :, :] - t1[:, s])
            term = jnp.concatenate([wsend[:, s]] * (pairs // 8), axis=0) * apart
            t2[:, s] = term
            share = share + term * apart
        return share

    ex2[1].wait_recv()
    moments.append(lane_sums(v2, y2) + last_terms(range(reach, links)))
    send_row(moments)
    near_sums = reduction(0, near)

    ex2[0].wait_recv()
    last_terms(range(reach))
    add_received(t2, y2, v3, False)

    for copies in (*ex0, *ex1, *ex2):
        copies.wait_send()
    near_sums.wait_recv()
    put_row(1, summed(0, group))
    far_sums = reduction(1, far)
    near_sums.wait_send()
    far_sums.wait_recv()
    high, low = (spread_row(x) for x in summed(1, others))
    m = [(high[i * pairs : (i + 1) * pairs], low[i * pairs : (i + 1) * pairs]) for i in range(6)]

    m0 = m[0][0]
    a0, over_a0 = m0 / m[1][0], m[1][0] / m0
    square, square_rest = two_product(a0, a0)
    double = 2.0 * a0

    def shifted(i):
        p, p_rest = two_product(m[i + 1][0], double)
        q, q_rest = two_product(m[i + 2][0], square)
        p_rest = p_rest + m[i + 1][1] * double
        q_rest = q_rest + (m[i + 2][1] * square + m[i + 2][0] * square_rest)
        s, s_rest = two_sum(m[i][0], -p)
        s, t_rest = two_sum(s, q)
        return s + ((s_rest + t_rest) + (m[i][1] - p_rest + q_rest))

    k0, k1, k2, k3 = (shifted(i) for i in range(4))

    b1 = k0 / m0
    a1 = k0 / (k1 - b1 * k0 * over_a0)
    v1q1 = -(k0 * over_a0 + k1) * over_a0
    r2q1 = k1 - a1 * (k2 + b1 * v1q1)
    rr2 = -a1 * r2q1
    b2 = rr2 / k0
    v1q2 = (v1q1 - k2) * over_a0
    r2q2 = k2 - a1 * (k3 + b1 * v1q2)
    r2ar2 = r2q1 - a1 * (r2q2 - b1 * r2q1 * over_a0)
    a2 = rr2 / (r2ar2 + b2 * r2q1)

    for s in tiles(nodes):
        w0, w1, w2, w3 = cur[:, s], v1[:, s], v2[:, s], v3[:, s]
        r1 = w0 - a0 * w1
        q1 = w1 - a0 * w2
        q2 = w2 - a0 * w3
        p1 = r1 + b1 * w0
        ap1 = q1 + b1 * w1
        r2 = r1 - a1 * ap1
        ar2 = q1 - a1 * (q2 + b1 * w2)
        p2 = r2 + b2 * p1
        ap2 = ar2 + b2 * ap1
        volt[:, s] = a0 * w0 + a1 * p1 + a2 * p2
        resid[:, s] = r2 - a2 * ap2

    far_sums.wait_send()


def write_out(volt, resid, volt_out, resid_out, sems):
    copies = [pltpu.make_async_copy(volt, volt_out, sems.at[0]), pltpu.make_async_copy(resid, resid_out, sems.at[1])]
    for copy in copies:
        copy.start()
    for copy in copies:
        copy.wait()


def solve(parts, group, currents, conductance, ground, ell_cols, send_rows):
    pairs, nodes = currents.shape
    links = send_rows.shape[0]
    bound = links * LANES
    others = parts // group
    most = max(group, others)
    field = pltpu.VMEM((pairs, nodes), F32)
    edge = pltpu.VMEM((pairs, bound), F32)
    vmem = pl.BlockSpec(memory_space=pltpu.VMEM)
    volt, resid = pl.pallas_call(
        functools.partial(kernel, parts, group),
        out_shape=(jax.ShapeDtypeStruct((pairs, nodes), F32),) * 2,
        in_specs=[pl.BlockSpec(memory_space=pltpu.HBM)] * 5,
        out_specs=(vmem, vmem),
        scratch_shapes=[
            field,
            pltpu.VMEM((1, nodes), F32),
            pltpu.VMEM((1, nodes), F32),
            pltpu.VMEM(ell_cols.shape, I32),
            pltpu.VMEM(send_rows.shape, I32),
            pltpu.SemaphoreType.DMA((5,)),
            pltpu.VMEM((nodes // LANES, nodes, LANES), BF16),
            pltpu.VMEM((nodes // LANES, 1, LANES), I32),
            field, field, field, field, field, field,
            pltpu.VMEM((1, nodes), F32),
            pltpu.VMEM((7 * pairs, nodes), BF16),
            pltpu.VMEM((8, bound), F32),
            pltpu.VMEM((links, bound, LANES), BF16),
            pltpu.VMEM((6 * pairs, bound), BF16),
            pltpu.VMEM((8, bound), F32),
            pltpu.VMEM((8, bound), F32),
            edge,
            edge, edge, edge, edge, edge, edge,
            pltpu.VMEM((links, pairs + 1, LANES), F32),
            pltpu.VMEM((links, pairs, LANES), F32),
            pltpu.VMEM((links, pairs, LANES), F32),
            pltpu.VMEM((links, pairs + 1, LANES), F32),
            pltpu.VMEM((links, pairs, LANES), F32),
            pltpu.VMEM((links, pairs, LANES), F32),
            pltpu.VMEM((2, most, 2, LANES), F32),
            pltpu.SemaphoreType.DMA((3,)),
            pltpu.SemaphoreType.DMA((3, 2)),
            pltpu.SemaphoreType.DMA((2,)),
            pltpu.SemaphoreType.DMA((2,)),
        ],
        compiler_params=pltpu.CompilerParams(
            collective_id=0, has_side_effects=True, vmem_limit_bytes=48 * 1024 * 1024
        ),
    )(*(pltpu.with_memory_space_constraint(x, pltpu.HBM) for x in (currents, conductance.reshape(1, nodes), ground.reshape(1, nodes), ell_cols, send_rows)))
    return pl.pallas_call(
        write_out,
        out_shape=(jax.ShapeDtypeStruct((pairs, nodes), F32),) * 2,
        in_specs=[vmem] * 2,
        out_specs=(pl.BlockSpec(memory_space=pltpu.HBM),) * 2,
        scratch_shapes=[pltpu.SemaphoreType.DMA((2,))],
        compiler_params=pltpu.CompilerParams(vmem_limit_bytes=1 << 20),
    )(volt, resid)


def solution(mesh):
    parts = mesh.shape["dom"]
    group = 16 if parts >= 256 else 4
    placed = (P(None, "dom"), P("dom"), P("dom"), P(None, "dom"), P("dom", None))
    return jax.shard_map(
        functools.partial(solve, parts, group),
        mesh=mesh,
        in_specs=placed,
        out_specs=(P(None, "dom"), P(None, "dom")),
        check_vma=False,
    )
```

```python
import functools

import jax
import jax.numpy as jnp
from jax import lax
from jax.experimental import pallas as pl
from jax.experimental.pallas import tpu as pltpu
from jax.sharding import PartitionSpec as P

MESH = pl.DeviceIdType.MESH
F32, BF16, I32 = jnp.float32, jnp.bfloat16, jnp.int32
LANES = 128
WIDE = 256
DIGITS = 8


def pieces(x):
    high = x.astype(BF16)
    rest = x - high.astype(F32)
    mid = rest.astype(BF16)
    low = (rest - mid.astype(F32)).astype(BF16)
    return [high, mid, low]


def joined(y, first, rows):
    return (y[first + 2 * rows : first + 3 * rows] + y[first + rows : first + 2 * rows]) + y[first : first + rows]


def two_sum(a, b):
    s = a + b
    part = s - a
    return s, (a - (s - part)) + (b - part)


def two_product(a, b):
    p = a * b
    wide_a, wide_b = a * 4097.0, b * 4097.0
    a1 = wide_a - (wide_a - a)
    b1 = wide_b - (wide_b - b)
    a2, b2 = a - a1, b - b1
    return p, ((a1 * b1 - p) + a1 * b2 + a2 * b1) + a2 * b2


def pair_add(a, b):
    s, e = two_sum(a[0], b[0])
    e = e + (a[1] + b[1])
    high = s + e
    return high, e - (high - s)


def tree(terms, add):
    while len(terms) > 1:
        terms = [add(a, b) for a, b in zip(terms[0::2], terms[1::2], strict=True)]
    return terms[0]


def tiles(width):
    return [slice(i, i + LANES) for i in range(0, width, LANES)]


def kernel(
    parts, group, cur_in, cond_in, gnd_in, ell_in, send_in, volt, resid,
    cur, cond, gnd, ell, send, in_sem, adj, from_slot, v1, v2, v3, y0, y1, y2, diag, lhs, wsend, mat, tlhs, c_at, d_at, z_at, u0, u1, u2, t0, t1, t2,
    out0, out1, out2, in0, in1, in2, red, ex_send, ex_recv, red_send, red_recv,
):
    pairs, nodes = cur.shape
    slots = ell.shape[0]
    links = send.shape[0]
    bound = links * LANES
    reach = links // 2
    offsets = list(range(-reach, 0)) + list(range(1, reach + 1))
    me = lax.axis_index("dom")
    others = parts // group
    mine, place = me // group, me % group

    assert reach == 3
    neighbours, landing, side_of = [], [], []
    for o, e in enumerate(offsets):
        d = abs(e)
        edge = me if e < 0 else parts - 1 - me
        spare = jnp.where(edge == 0, 1 if d < 3 else 2, 0)
        spare_d = jnp.where(edge == 0, min(d + 1, 3), jnp.where(edge == 1, d - 1, 3))
        inside = edge >= d
        spare_peer = spare if e < 0 else parts - 1 - spare
        spare_slot = reach - spare_d if e < 0 else reach - 1 + spare_d
        neighbours.append(jnp.where(inside, me + e, spare_peer))
        landing.append(jnp.where(inside, links - 1 - o, spare_slot))
        side_of.append(jnp.where(inside, 1 if e < 0 else 0, 0 if e < 0 else 1))
    def steps(d, count):
        return min(d, count - d)

    near = [
        (d, mine * group + lax.rem(place + d, group))
        for d in sorted(range(1, group), key=lambda d: -steps(d, group))
    ]
    side = 4 if others == 16 else 2
    row, column = mine // side, mine % side
    far = [
        (d, (lax.rem(row + d // side, side) * side + lax.rem(column + d % side, side)) * group + place)
        for d in sorted(range(1, others), key=lambda d: -steps(d // side, side) - steps(d % side, side))
    ]

    loads = [
        pltpu.make_async_copy(source, target, in_sem.at[i])
        for i, (source, target) in enumerate(
            ((cur_in, cur), (cond_in, cond), (gnd_in, gnd), (ell_in, ell), (send_in, send))
        )
    ]
    loads[4].start()
    loads[0].start()
    for i in range(1, 4):
        loads[i].start()

    barrier = pltpu.get_barrier_semaphore()
    for peer in neighbours + [peer for _, peer in near + far]:
        pl.semaphore_signal(barrier, inc=1, device_id={"dom": peer}, device_id_type=MESH)
    word_ids = lax.broadcasted_iota(I32, (8, LANES), 0)
    no_word = jnp.zeros((8, LANES), I32)
    words = nodes // DIGITS

    def taken(x, lane):
        return jnp.take_along_axis(x, lane, axis=1, mode="promise_in_bounds")

    def places(o):
        node = jnp.broadcast_to(send[o : o + 1, :], (8, LANES))
        return node & (LANES - 1), lax.shift_right_arithmetic(node, 7)

    def picked(source, rows):
        found = []
        for o in range(links):
            lane, tile = places(o)
            parts_found = [jnp.zeros((8, LANES), F32)] * (rows // 8)
            for k, s in enumerate(tiles(nodes)):
                here = tile == k
                for i in range(rows // 8):
                    parts_found[i] = jnp.where(here, taken(source(i, s), lane), parts_found[i])
            found.append(jnp.concatenate(parts_found, axis=0))
        return found

    def field_rows(field):
        return lambda i, s: field[i * 8 : i * 8 + 8, s]

    with jax.named_scope("pick_cur"):
        loads[4].wait()
        loads[0].wait()
        loads[1].wait()
        for o, (u, c) in enumerate(
            zip(
                picked(field_rows(cur), pairs),
                picked(lambda i, s: jnp.broadcast_to(cond[:, s], (8, LANES)), 8),
                strict=True,
            )
        ):
            s = slice(o * LANES, (o + 1) * LANES)
            u0[:, s] = u
            wsend[:, s] = c
            c_at[:, s] = c
            out0[o, 0:pairs, :] = u
            out0[o, pairs : pairs + 1, :] = c[0:1]

    def send_all(step, out, into):
        for o in sorted(range(links), key=lambda o: -abs(offsets[o])):
            pltpu.make_async_remote_copy(
                src_ref=out.at[o],
                dst_ref=into.at[landing[o]],
                send_sem=ex_send.at[step],
                recv_sem=ex_recv.at[step, side_of[o]],
                device_id={"dom": neighbours[o]},
                device_id_type=MESH,
            ).start()

    def exchange(step, out, into):
        return [
            pltpu.make_async_remote_copy(
                src_ref=out.at[half], dst_ref=into.at[half], send_sem=ex_send.at[step], recv_sem=ex_recv.at[step, i],
                device_id={"dom": neighbours[0]}, device_id_type=MESH,
            )
            for i, half in enumerate((slice(0, reach), slice(reach, links)))
        ]

    def fill_counts(into, g, p, count, digits):
        word = list(p)
        for i in range(slots):
            for j in range(i):
                same = g[i] == g[j]
                word[i] = word[i] + jnp.where(same, p[j], no_word)
                word[j] = word[j] + jnp.where(same, p[i], no_word)
        for h in range(0, count, 64):
            chunk = []
            for q in range(h, h + 64, 8):
                ids = word_ids + q
                acc = no_word
                for s in range(slots):
                    acc = jnp.where(g[s] == ids, word[s], acc)
                chunk.append(acc)
            chunk = jnp.concatenate(chunk, axis=0)
            for r in range(digits):
                last = r == DIGITS - 1
                digit = lax.shift_right_logical(chunk, 4 * r) if last else chunk & (15 << (4 * r))
                into[r * count + h : r * count + h + 64, :] = digit.astype(F32).astype(BF16)

    def build(t, _):
        off = pl.multiple_of(t * LANES, LANES)
        block = ell[:, pl.ds(off, LANES)]
        local = (block >= 0) & (block < nodes)
        wide_g = jnp.where(local, block & (words - 1), -1)
        wide_p = jnp.left_shift(jnp.ones_like(block), jnp.where(local, (block // words) * 4, 0))
        g = [jnp.broadcast_to(wide_g[s : s + 1, :], (8, LANES)) for s in range(slots)]
        p = [jnp.broadcast_to(wide_p[s : s + 1, :], (8, LANES)) for s in range(slots)]
        fill_counts(adj.at[t], g, p, words, DIGITS)
        from_slot[t] = jnp.max(block, axis=0, keepdims=True) - nodes
        return 0

    def adj_block(b):
        return jnp.concatenate([adj[b // LANES], adj[b // LANES + 1]], axis=1)

    def scale_of(r):
        return 1.0 if r == DIGITS - 1 else 16.0**-r

    def split_part(value, s):
        part = value * scale_of(s.start // words)
        for i, piece in enumerate(pieces(part)):
            lhs[i * pairs : (i + 1) * pairs, s] = piece
        for i, piece in enumerate(pieces(part * cond[:, s])):
            lhs[(3 + i) * pairs : (4 + i) * pairs, s] = piece

    half = 0.5
    with jax.named_scope("adj_a"):
        loads[3].wait()
        part_of = jnp.where(row == 0, 16, jnp.where(row == 1, 10, 4))
        ahead = jnp.where(place < group // 2, nodes // LANES, nodes // LANES * part_of // 16)
        lax.fori_loop(0, ahead, build, 0)
    with jax.named_scope("barwait"):
        pl.semaphore_wait(barrier, len(neighbours) + len(near) + len(far))
    send_all(0, out0, in0)
    ex0 = exchange(0, out0, in0)
    with jax.named_scope("adj_b"):
        lax.fori_loop(ahead, nodes // LANES, build, 0)

    def local_operator(v, y, first, u=None, out=None):
        if u is not None:
            listed = [places(o) for o in range(links)]
            found = [[jnp.zeros((8, LANES), F32)] * (pairs // 8) for _ in range(links)]
        rows = 7 * pairs if first else 6 * pairs
        for b in range(0, nodes, WIDE):
            s = slice(b, b + WIDE)
            prod = jnp.dot(lhs[0:rows, :], adj_block(b), preferred_element_type=F32)
            c = cond[:, s]
            if first:
                extra = prod[6 * pairs :]
                around = joined(extra, 0, 1)
                diag[:, s] = gnd[:, s] + half * (c * extra[3:4] + around)
            result = diag[:, s] * v[:, s] - half * (c * joined(prod, 0, pairs) + joined(prod, 3 * pairs, pairs))
            y[:, s] = result
            if u is not None:
                for k in (b // LANES, b // LANES + 1):
                    inner = k * LANES - b
                    for o, (lane, tile) in enumerate(listed):
                        here = tile == k
                        for i in range(pairs // 8):
                            piece = result[i * 8 : i * 8 + 8, inner : inner + LANES]
                            found[o][i] = jnp.where(here, taken(piece, lane), found[o][i])
        if u is not None:
            for o in range(links):
                both = jnp.concatenate(found[o], axis=0)
                u[:, o * LANES : (o + 1) * LANES] = both
                if out is not None:
                    out[o, :, :] = both

    def add_received(t, y, v, onward):
        for k, s in enumerate(tiles(nodes)):
            slot = jnp.broadcast_to(from_slot[k], (8, LANES))
            lane, link = slot & (LANES - 1), lax.shift_right_arithmetic(slot, 7)
            found = [jnp.zeros((8, LANES), F32)] * (pairs // 8)
            for o, part in enumerate(tiles(bound)):
                here = link == o
                for i in range(pairs // 8):
                    found[i] = jnp.where(here, taken(t[i * 8 : i * 8 + 8, part], lane), found[i])
            value = y[:, s] + jnp.concatenate(found, axis=0)
            v[:, s] = value
            if onward:
                split_part(value, s)

    def lane_sums(first, second):
        total = None
        for s in tiles(first.shape[1]):
            term = first[:, s] * second[:, s]
            total = term if total is None else total + term
        return total

    def send_row(sums):
        blocks = jnp.concatenate(sums + [jnp.zeros((LANES - pairs * len(sums), LANES), F32)], axis=0)
        turned = jnp.transpose(blocks)
        total = tree([two_sum(turned[i : i + 8], turned[i + 8 : i + 16]) for i in range(0, LANES, 16)], pair_add)
        for shift in (4, 2, 1):
            total = pair_add(total, tuple(pltpu.roll(x, shift, axis=0) for x in total))
        put_row(0, total)

    def put_row(stage, total):
        red[stage, 0, 0:1, :] = total[0][0:1]
        red[stage, 0, 1:2, :] = total[1][0:1]

    def reduction(stage, peers):
        for d, peer in peers:
            pltpu.make_async_remote_copy(
                src_ref=red.at[stage, 0],
                dst_ref=red.at[stage, d],
                send_sem=red_send.at[stage],
                recv_sem=red_recv.at[stage],
                device_id={"dom": peer},
                device_id_type=MESH,
            ).start()
        slots_used = red.at[stage, 1 : len(peers) + 1]
        return pltpu.make_async_remote_copy(
            src_ref=slots_used, dst_ref=slots_used, send_sem=red_send.at[stage], recv_sem=red_recv.at[stage],
            device_id={"dom": peers[0][1]}, device_id_type=MESH,
        )

    def summed(stage, count):
        return tree([(red[stage, d, 0:1, :], red[stage, d, 1:2, :]) for d in range(count)], pair_add)

    def spread_row(row):
        return jnp.transpose(jnp.broadcast_to(row, (LANES, LANES)))

    lhs[6 * pairs :, :] = jnp.zeros((pairs, nodes), BF16)
    loads[2].wait()
    for r in range(DIGITS):
        s = slice(r * words, (r + 1) * words)
        for i, piece in enumerate(pieces(cond[:, s] * scale_of(r))):
            lhs[6 * pairs + i : 6 * pairs + i + 1, s] = piece
        lhs[6 * pairs + 3 : 6 * pairs + 4, s] = jnp.full((1, words), scale_of(r), BF16)
    for s in tiles(nodes):
        split_part(cur[:, s], s)
    local_operator(cur, y0, True, u1, out1)
    send_all(1, out1, in1)
    ex1 = exchange(1, out1, in1)

    def remote_terms(u, other, t):
        for o in range(links):
            s = slice(o * LANES, (o + 1) * LANES)
            weight = jnp.concatenate([wsend[:, s]] * (pairs // 8), axis=0)
            t[:, s] = weight * (u[:, s] - other(o, s))

    early = place < 4

    @pl.when(early)
    def _():
        with jax.named_scope("prep"):
            for o, d in enumerate(picked(lambda i, s: jnp.broadcast_to(diag[:, s], (8, LANES)), 8)):
                d_at[:, o * LANES : (o + 1) * LANES] = d
            for s in tiles(nodes):
                split_part(y0[:, s], s)
            local_operator(y0, y1, False, z_at)
            spans = [(0, 8)] + [(i, i + 1) for i in range(8, slots)]
            for o in range(links):
                lane, tile = places(o)
                g, p = [], []
                for first, end in spans:
                    near_by = jnp.full((8, LANES), -1, I32)
                    for k, s in enumerate(tiles(nodes)):
                        rows = jnp.broadcast_to(ell[first:end, s], (8, LANES))
                        near_by = jnp.where(tile == k, taken(rows, lane), near_by)
                    inner = near_by & (LANES - 1)
                    outer = jnp.where(near_by < nodes, lax.shift_right_arithmetic(near_by, 7), -1)
                    slot = jnp.full((8, LANES), -1, I32)
                    for k in range(nodes // LANES):
                        known = jnp.broadcast_to(from_slot[k], (8, LANES))
                        slot = jnp.where(outer == k, taken(known, inner), slot)
                    word = jnp.where(slot >= 0, slot & (LANES - 1), -1)
                    power = jnp.left_shift(
                        jnp.ones_like(slot), jnp.where(slot >= 0, lax.shift_right_arithmetic(slot, 7) * 4, 0)
                    )
                    for i in range(end - first):
                        g.append(jnp.broadcast_to(word[i : i + 1], (8, LANES)))
                        p.append(jnp.broadcast_to(power[i : i + 1], (8, LANES)))
                fill_counts(mat.at[o], g, p, LANES, links)

    ex0[0].wait_recv()
    ex0[1].wait_recv()
    for o in range(links):
        s = slice(o * LANES, (o + 1) * LANES)
        live = jnp.broadcast_to(send[o : o + 1, :], (8, LANES)) >= 0
        wsend[:, s] = jnp.where(live, half * (wsend[:, s] + in0[o, pairs : pairs + 1, :]), 0.0)
    remote_terms(u0, lambda o, s: in0[o, 0:pairs, :], t0)
    def both_halves(x):
        return jnp.concatenate([x] * (pairs // 8), axis=0)

    @pl.when(early)
    def _():
        with jax.named_scope("short"):
            for r, s in enumerate(tiles(bound)):
                part = t0[:, s] * 16.0**-r
                for i, piece in enumerate(pieces(part)):
                    tlhs[i * pairs : (i + 1) * pairs, s] = piece
                for i, piece in enumerate(pieces(part * both_halves(c_at[:, s]))):
                    tlhs[(3 + i) * pairs : (4 + i) * pairs, s] = piece
            for b in range(0, bound, WIDE):
                counts = jnp.concatenate([mat[b // LANES], mat[b // LANES + 1]], axis=1)
                prod = jnp.dot(tlhs[...], counts, preferred_element_type=F32)
                for o in (b // LANES, b // LANES + 1):
                    s = slice(o * LANES, (o + 1) * LANES)
                    half_prod = prod[:, o * LANES - b : (o + 1) * LANES - b]
                    around = both_halves(c_at[:, s]) * joined(half_prod, 0, pairs)
                    around = around + joined(half_prod, 3 * pairs, pairs)
                    value = z_at[:, s] + (both_halves(d_at[:, s]) * t0[:, s] - half * around)
                    u2[:, s] = value
                    out2[o, :, :] = value
            send_all(2, out2, in2)

    add_received(t0, y0, v1, True)

    @pl.when(early)
    def _():
        local_operator(v1, y1, False)

    @pl.when(jnp.logical_not(early))
    def _():
        local_operator(v1, y1, False, u2, out2)
        send_all(2, out2, in2)

    ex2 = exchange(2, out2, in2)
    moments = [lane_sums(cur, cur), lane_sums(cur, v1), lane_sums(v1, v1)]

    ex1[0].wait_recv()
    ex1[1].wait_recv()
    u1[...] = u1[...] + t0[...]
    remote_terms(u1, lambda o, s: in1[o, :, :] - t0[:, s], t1)
    add_received(t1, y1, v2, True)
    moments += [lane_sums(v1, v2), lane_sums(v2, v2)]
    local_operator(v2, y2, False)

    def last_terms(side):
        share = jnp.zeros((pairs, LANES), F32)
        for o in side:
            s = slice(o * LANES, (o + 1) * LANES)
            here = u2[:, s] + t1[:, s]
            apart = here - (in2[o, :, :] - t1[:, s])
            term = jnp.concatenate([wsend[:, s]] * (pairs // 8), axis=0) * apart
            t2[:, s] = term
            share = share + term * apart
        return share

    ex2[1].wait_recv()
    moments.append(lane_sums(v2, y2) + last_terms(range(reach, links)))
    send_row(moments)
    near_sums = reduction(0, near)

    ex2[0].wait_recv()
    last_terms(range(reach))
    add_received(t2, y2, v3, False)

    for copies in (*ex0, *ex1, *ex2):
        copies.wait_send()
    near_sums.wait_recv()
    put_row(1, summed(0, group))
    far_sums = reduction(1, far)
    near_sums.wait_send()
    far_sums.wait_recv()
    high, low = (spread_row(x) for x in summed(1, others))
    m = [(high[i * pairs : (i + 1) * pairs], low[i * pairs : (i + 1) * pairs]) for i in range(6)]

    m0 = m[0][0]
    a0, over_a0 = m0 / m[1][0], m[1][0] / m0
    square, square_rest = two_product(a0, a0)
    double = 2.0 * a0

    def shifted(i):
        p, p_rest = two_product(m[i + 1][0], double)
        q, q_rest = two_product(m[i + 2][0], square)
        p_rest = p_rest + m[i + 1][1] * double
        q_rest = q_rest + (m[i + 2][1] * square + m[i + 2][0] * square_rest)
        s, s_rest = two_sum(m[i][0], -p)
        s, t_rest = two_sum(s, q)
        return s + ((s_rest + t_rest) + (m[i][1] - p_rest + q_rest))

    k0, k1, k2, k3 = (shifted(i) for i in range(4))

    b1 = k0 / m0
    a1 = k0 / (k1 - b1 * k0 * over_a0)
    v1q1 = -(k0 * over_a0 + k1) * over_a0
    r2q1 = k1 - a1 * (k2 + b1 * v1q1)
    rr2 = -a1 * r2q1
    b2 = rr2 / k0
    v1q2 = (v1q1 - k2) * over_a0
    r2q2 = k2 - a1 * (k3 + b1 * v1q2)
    r2ar2 = r2q1 - a1 * (r2q2 - b1 * r2q1 * over_a0)
    a2 = rr2 / (r2ar2 + b2 * r2q1)

    wide = 1.0 + b1
    slope = a0 + a1 * wide
    c0 = slope + a2 * (1.0 + b2 * wide)
    c1 = -(a1 * a0) - a2 * (slope + b2 * a0)
    c2 = a2 * (a1 * a0)
    for s in tiles(nodes):
        w0, w1, w2, w3 = cur[:, s], v1[:, s], v2[:, s], v3[:, s]
        volt[:, s] = c0 * w0 + c1 * w1 + c2 * w2
        resid[:, s] = w0 - (c0 * w1 + c1 * w2 + c2 * w3)

    far_sums.wait_send()


def write_out(volt, resid, volt_out, resid_out, sems):
    copies = [pltpu.make_async_copy(volt, volt_out, sems.at[0]), pltpu.make_async_copy(resid, resid_out, sems.at[1])]
    for copy in copies:
        copy.start()
    for copy in copies:
        copy.wait()


def solve(parts, group, currents, conductance, ground, ell_cols, send_rows):
    pairs, nodes = currents.shape
    links = send_rows.shape[0]
    bound = links * LANES
    others = parts // group
    most = max(group, others)
    field = pltpu.VMEM((pairs, nodes), F32)
    edge = pltpu.VMEM((pairs, bound), F32)
    vmem = pl.BlockSpec(memory_space=pltpu.VMEM)
    volt, resid = pl.pallas_call(
        functools.partial(kernel, parts, group),
        out_shape=(jax.ShapeDtypeStruct((pairs, nodes), F32),) * 2,
        in_specs=[pl.BlockSpec(memory_space=pltpu.HBM)] * 5,
        out_specs=(vmem, vmem),
        scratch_shapes=[
            field,
            pltpu.VMEM((1, nodes), F32),
            pltpu.VMEM((1, nodes), F32),
            pltpu.VMEM(ell_cols.shape, I32),
            pltpu.VMEM(send_rows.shape, I32),
            pltpu.SemaphoreType.DMA((5,)),
            pltpu.VMEM((nodes // LANES, nodes, LANES), BF16),
            pltpu.VMEM((nodes // LANES, 1, LANES), I32),
            field, field, field, field, field, field,
            pltpu.VMEM((1, nodes), F32),
            pltpu.VMEM((7 * pairs, nodes), BF16),
            pltpu.VMEM((8, bound), F32),
            pltpu.VMEM((links, bound, LANES), BF16),
            pltpu.VMEM((6 * pairs, bound), BF16),
            pltpu.VMEM((8, bound), F32),
            pltpu.VMEM((8, bound), F32),
            edge,
            edge, edge, edge, edge, edge, edge,
            pltpu.VMEM((links, pairs + 1, LANES), F32),
            pltpu.VMEM((links, pairs, LANES), F32),
            pltpu.VMEM((links, pairs, LANES), F32),
            pltpu.VMEM((links, pairs + 1, LANES), F32),
            pltpu.VMEM((links, pairs, LANES), F32),
            pltpu.VMEM((links, pairs, LANES), F32),
            pltpu.VMEM((2, most, 2, LANES), F32),
            pltpu.SemaphoreType.DMA((3,)),
            pltpu.SemaphoreType.DMA((3, 2)),
            pltpu.SemaphoreType.DMA((2,)),
            pltpu.SemaphoreType.DMA((2,)),
        ],
        compiler_params=pltpu.CompilerParams(
            collective_id=0, has_side_effects=True, vmem_limit_bytes=48 * 1024 * 1024
        ),
    )(*(pltpu.with_memory_space_constraint(x, pltpu.HBM) for x in (currents, conductance.reshape(1, nodes), ground.reshape(1, nodes), ell_cols, send_rows)))
    return pl.pallas_call(
        write_out,
        out_shape=(jax.ShapeDtypeStruct((pairs, nodes), F32),) * 2,
        in_specs=[vmem] * 2,
        out_specs=(pl.BlockSpec(memory_space=pltpu.HBM),) * 2,
        scratch_shapes=[pltpu.SemaphoreType.DMA((2,))],
        compiler_params=pltpu.CompilerParams(vmem_limit_bytes=1 << 20),
    )(volt, resid)


def solution(mesh):
    parts = mesh.shape["dom"]
    group = 16 if parts >= 256 else 4
    placed = (P(None, "dom"), P("dom"), P("dom"), P(None, "dom"), P("dom", None))
    return jax.shard_map(
        functools.partial(solve, parts, group),
        mesh=mesh,
        in_specs=placed,
        out_specs=(P(None, "dom"), P(None, "dom")),
        check_vma=False,
    )
```
